256 devices in a mesh: pix: 128 (over x_hi, z, y, core), tm: 2 (over x_lo).
Axes of the slice: x: 4 (x_hi: 2, x_lo: 2; x = x_hi * 2 + x_lo), y: 4, z: 8, core: 2. Of those that a mesh axis runs over, the one named last changes fastest.
Arguments:
- iq: bfloat16 [600, 2, 524288], P('tm', None, 'pix'), as said below
- tail_frames: bfloat16 [150, 2, 524288], P(None, None, 'pix'), as said below
- start_basis: float32 [300, 128], replicated, may hold values from -6 to 6
- low_rank: int32 [4], P('tm'), may hold values from 1 to 32
- high_rank: int32 [4], P('tm'), may hold values from 64 to 128
Outputs:
- power: float32 [4, 524288], P('tm', 'pix')
- basis: float32 [4, 300, 128], P('tm')
The draws below stay inside these ranges and needn't reach their ends.
Inputs may be any that keep to these rules, and one draw needn't show every extreme that they name: low_rank[w] < high_rank[w] <= 128 for every window. `iq`: real-valued samples of order one. `tail_frames`: real-valued samples of order one, continuing iq.
All inputs are finite; a program needn't handle non-finite values.
Results may differ from the reference program's by a relative error of at most 0.0008.
Values may be sent and summed in bfloat16 or wider, within the bound.
No kernel may reach another device: no remote copies, remote signals or barrier semaphores. Data moves between devices by JAX's collectives and lax.ppermute only.
A program may use at most 128 MiB of HBM per device.

```python
import math
import jax
import jax.numpy as jnp
from jax import lax

W = 300
HOP = 150
K = 128
ITERS = 3
PIX_DEV = 4096
NPIX = 524288
NWIN = 4
FRAMES = 600


def acquisition(key):
    base = jax.random.fold_in(key, 11)
    keys = jax.random.split(base, 6)
    total = FRAMES + HOP
    noise = jax.random.normal(keys[0], (total, 2, NPIX), jnp.float32)
    scale = jnp.exp(jax.random.uniform(keys[1], (NPIX,), jnp.float32, math.log(0.5), math.log(3.0)))
    blocks = NPIX // PIX_DEV
    gain = jnp.exp(jax.random.uniform(keys[2], (total, blocks), jnp.float32, math.log(0.5), math.log(2.0)))
    gain = jnp.repeat(gain, PIX_DEV, axis=1)
    omega = jax.random.uniform(keys[3], (4,), jnp.float32, 0.002, 0.03)
    amplitude = 0.3 * jax.random.normal(keys[4], (4, NPIX), jnp.float32)
    phase = jax.random.uniform(keys[5], (4, NPIX), jnp.float32, -math.pi, math.pi)
    frame = jnp.arange(total, dtype=jnp.float32)[:, None]
    real_part = jnp.zeros((total, NPIX), jnp.float32)
    imag_part = jnp.zeros((total, NPIX), jnp.float32)
    for index in range(4):
        angle = omega[index] * frame + phase[index][None, :]
        real_part = real_part + amplitude[index][None, :] * jnp.cos(angle)
        imag_part = imag_part + amplitude[index][None, :] * jnp.sin(angle)
    clutter = jnp.stack([real_part, imag_part], axis=1)
    return (noise * gain[:, None, :] + clutter) * scale[None, None, :]


def draw_iq(key, part):
    return acquisition(key)[:FRAMES].astype(jnp.bfloat16)


def draw_tail_frames(key, part):
    return acquisition(key)[FRAMES:].astype(jnp.bfloat16)


def place_ends(result, rng, smallest, top_value):
    place = [jax.random.randint(jax.random.fold_in(rng, axis), (), 0, length) for axis, length in enumerate(result.shape)]
    longest = result.shape.index(max(result.shape))
    neighbour = place[:longest] + [(place[longest] + 1) % result.shape[longest]] + place[longest + 1:]
    return result.at[tuple(place)].set(smallest).at[tuple(neighbour)].set(top_value)


def normal_values(own_key, shape, deviation, limit, held_as=jnp.bfloat16):
    values = jax.random.normal(own_key, shape, jnp.float32) * deviation
    return jnp.minimum(jnp.maximum(values, -limit), limit).astype(held_as)


def setup_inputs(seed: int = 0) -> dict:
    streams_of = jax.random.split(jax.random.key(seed), 6)
    return {
        "iq": draw_iq(jax.random.fold_in(streams_of[5], 71), 0),
        "tail_frames": draw_tail_frames(jax.random.fold_in(streams_of[5], 71), 0),
        "start_basis": normal_values(streams_of[2], (W, K), 1.0, 6.0, jnp.float32),
        "low_rank": place_ends(jax.random.randint(streams_of[3], (NWIN,), 1, K // 4 + 1), jax.random.fold_in(streams_of[3], 1), 1, (K // 4 + 1) - 1).astype(jnp.int32),
        "high_rank": place_ends(jax.random.randint(streams_of[4], (NWIN,), K // 2, K + 1), jax.random.fold_in(streams_of[4], 1), K // 2, K).astype(jnp.int32),
    }


def iterate(gram, start):
    basis = start
    for step in range(ITERS):
        image = jnp.dot(gram, basis, precision=lax.Precision.HIGHEST)
        inner = jnp.dot(image.T, image, precision=lax.Precision.HIGHEST)
        factor = jnp.linalg.cholesky(inner)
        basis = lax.linalg.triangular_solve(factor, image, left_side=False, lower=True, transpose_a=True)
    return basis

def reference(iq, tail_frames, start_basis, low_rank, high_rank):
    extended = jnp.concatenate([iq, tail_frames], axis=0)
    columns = jnp.arange(K, dtype=jnp.int32)
    powers = []
    bases = []
    for window in range(NWIN):
        casorati = extended[window * HOP:window * HOP + W].reshape(W, 2 * NPIX)
        gram = jnp.dot(casorati.astype(jnp.float32), casorati.T.astype(jnp.float32), preferred_element_type=jnp.float32)
        basis = iterate(gram, start_basis)
        keep = ((columns >= low_rank[window]) & (columns < high_rank[window])).astype(jnp.float32)
        proj = jnp.dot(basis * keep[None, :], basis.T, precision=lax.Precision.HIGHEST).astype(jnp.bfloat16)
        filtered = jnp.dot(proj.astype(jnp.float32), casorati.astype(jnp.float32), preferred_element_type=jnp.float32)
        powers.append(jnp.sum((filtered * filtered).reshape(W, 2, NPIX), axis=(0, 1)) / W)
        bases.append(basis)
    return (jnp.stack(powers), jnp.stack(bases))
```

```python
import functools

import jax
import jax.numpy as jnp
from jax import lax
from jax.experimental import pallas as pl
from jax.experimental.pallas import tpu as pltpu
from jax.sharding import Mesh
from jax.sharding import PartitionSpec as P

K = 128
ITERS = 3
WINDOW = 300
HALF = 150
MAIN = 128
REM = HALF - MAIN
SPAN = 384
USED = 320
TILE = 32
PACKED = 512
HI = lax.Precision.HIGHEST
F32 = jnp.float32
BF16 = jnp.bfloat16
PIX = ("pix_0", "pix_1", "pix_2", "pix_3")
CHIPS = ("pix_0", "pix_1", "pix_2")
SMEM = pl.BlockSpec(memory_space=pltpu.SMEM)
VMEM = pl.BlockSpec(memory_space=pltpu.VMEM)


def grid_of(shape, axis):
    return lax.broadcasted_iota(jnp.int32, shape, axis)


def across(a, b):
    return lax.dot_general(a, b, (((1,), (1,)), ((), ())), preferred_element_type=F32)


def pack(out, first, cross, second):
    row = grid_of((MAIN, 128), 0)
    lane = grid_of((MAIN, 128), 1)
    zero = jnp.zeros((152, 128), F32)
    one = zero if first is None else first[:, 128:256]
    two = zero if cross is None else pltpu.roll(cross[:, 128:256], 32, 1)
    three = zero if second is None else pltpu.roll(second[:, 128:256], 64, 1)
    upper = zero[:MAIN] if first is None else first[0:MAIN, 0:128]
    lower = zero[:MAIN] if second is None else second[0:MAIN, 0:128]
    out[0:MAIN, :] = jnp.where(lane >= row, upper, lower)
    out[128:280, :] = zero if cross is None else cross[:, 0:128]
    out[280:432, :] = one + two + three
    out[432:440, :] = jnp.where(
        grid_of((8, 128), 0) == 0,
        jnp.sum(jnp.where(lane == row, lower, 0.0), axis=0, keepdims=True),
        0.0,
    )
    out[440:, :] = jnp.zeros((PACKED - 440, 128), F32)


def local_kernel(place, frames, tail, even, odd, extra, sums):
    step = pl.program_id(0)

    @pl.when(step == 0)
    def _():
        sums[...] = jnp.zeros_like(sums)

    for part in range(2):
        a = frames[part, 0]
        b = frames[part, 1]
        c = tail[part]
        for index, (left, right) in enumerate(((a, a), (a, b), (b, b), (b, c), (c, c))):
            sums[index, 0:HALF, 0:HALF] += across(left, right)

    @pl.when(step == pl.num_programs(0) - 1)
    def _():
        pack(even, sums[0], sums[1], sums[2])
        scale = place[1].astype(F32)
        pack(odd, sums[2], sums[3] * scale, sums[4] * scale)
        pack(extra, None, None, sums[0])


def local_products(place, frames, tail):
    pixels = frames.shape[-1]
    steps = 4
    width = pixels // steps
    out = jax.ShapeDtypeStruct((PACKED, 128), F32)
    whole = pl.BlockSpec((PACKED, 128), lambda i: (0, 0))
    return pl.pallas_call(
        local_kernel,
        grid=(steps,),
        out_shape=(out, out, out),
        in_specs=[
            SMEM,
            pl.BlockSpec((2, 2, HALF, width), lambda i: (0, 0, 0, i)),
            pl.BlockSpec((2, HALF, width), lambda i: (0, 0, i)),
        ],
        out_specs=(whole, whole, whole),
        scratch_shapes=[pltpu.VMEM((5, 152, 256), F32)],
        cost_estimate=pl.CostEstimate(flops=4 * 10**9, bytes_accessed=8 * 10**6, transcendentals=0),
        name="local_products",
    )(place, frames, tail)


def cross_kernel(place, frames, arrived, even, odd, extra, keep, swap, send, sums, mix):
    last = place[1] == 1
    half = arrived.shape[-1]
    total = jnp.zeros((HALF, HALF), F32)
    for part in range(2):
        got = arrived[part]
        left = jnp.where(last, got, frames[part, 1, :, 0:half])
        right = jnp.where(last, frames[part, 0, :, half:], got)
        total += across(left, right)
    sums[...] = jnp.zeros_like(sums)
    sums[0:HALF, 0:HALF] = total
    pack(mix, None, sums[...], None)
    later = odd[...] + jnp.where(last, 0.0, mix[...])
    sooner = even[...]
    core = place[0] == 1
    keep[...] = jnp.where(core, later, sooner)
    swap[...] = jnp.where(core, sooner, later)
    send[...] = extra[...] + mix[...]


def cross_products(place, frames, arrived, even, odd, extra):
    out = jax.ShapeDtypeStruct((PACKED, 128), F32)
    return pl.pallas_call(
        cross_kernel,
        out_shape=(out, out, out),
        in_specs=[SMEM] + [VMEM] * 5,
        out_specs=(VMEM, VMEM, VMEM),
        scratch_shapes=[pltpu.VMEM((152, 256), F32), pltpu.VMEM((PACKED, 128), F32)],
        name="cross_products",
    )(place, frames, arrived, even, odd, extra)


def unpack(rows, gram):
    row = grid_of((128, 128), 0)
    lane = grid_of((128, 128), 1)
    both = rows[0:128]
    turned = both.T
    gram[0:128, 0:128] = jnp.where(lane >= row, both, turned)
    gram[128:256, 128:256] = jnp.where(
        lane < row, both, jnp.where(lane == row, rows[432:433], turned)
    )
    cross = rows[128:256]
    gram[0:128, 128:256] = cross
    gram[128:256, 0:128] = cross.T
    side = rows[280:408]
    turn = jnp.concatenate([rows[256:280], jnp.zeros((104, 128), F32)], axis=0).T
    first = jnp.where(lane < 64, side, 0.0)
    second = jnp.where(lane < 32, turn, jnp.where(lane < 64, pltpu.roll(side, 96, 1), 0.0))
    gram[0:128, 256:384] = first
    gram[128:256, 256:384] = second
    gram[256:384, 0:128] = first.T
    gram[256:384, 128:256] = second.T
    corner = rows[408:432]
    gram[256:384, 256:384] = jnp.zeros((128, 128), F32)
    short = grid_of((24, 128), 1)
    gram[256:280, 256:384] = jnp.where(short < 64, corner, 0.0)
    moved = pltpu.roll(corner, 96, 1)
    square = jnp.concatenate(
        [jnp.where(short < 32, moved, 0.0), jnp.zeros((104, 128), F32)], axis=0
    ).T[0:24]
    gram[288:312, 256:384] = jnp.where(
        short < 32, square, jnp.where(short < 64, moved, 0.0)
    )


def row_of(vector, index):
    return jnp.broadcast_to(vector[index : index + 1, :], vector.shape)


def eliminate(work, step):
    first = TILE * step
    sub = grid_of((8, 128), 0)
    lane = grid_of((8, 128), 1)
    groups = TILE // 8
    cols = {}
    for g in range(groups):
        top = first + 8 * g
        block = work[top : top + 8, 0:128]
        for k in range(8 * (g + 1)):
            at = first + k
            cols[g, k] = jnp.broadcast_to(block[:, at : at + 1], (8, 128))
    inverse = [jnp.where(lane == sub + 8 * g, 1.0, 0.0).astype(F32) for g in range(groups)]
    for j in range(TILE):
        gj, rj = divmod(j, 8)
        scale = lax.rsqrt(row_of(cols[gj, j], rj))
        for g in range(gj, groups):
            cols[g, j] = cols[g, j] * scale
        for k in range(j + 1, TILE):
            gk, rk = divmod(k, 8)
            factor = row_of(cols[gk, j], rk)
            for g in range(gk, groups):
                cols[g, k] = cols[g, k] - cols[g, j] * factor
        pivot = row_of(inverse[gj], rj) * scale
        for g in range(gj, groups):
            if g == gj:
                below = jnp.where(sub > rj, cols[g, j], 0.0)
                inverse[g] = jnp.where(sub == rj, pivot, inverse[g] - below * pivot)
            else:
                inverse[g] = inverse[g] - cols[g, j] * pivot
    lhs = jnp.concatenate(inverse, axis=0)[:, 0:TILE]
    rows = jnp.dot(
        lhs, work[first : first + TILE, :], precision=HI, preferred_element_type=F32
    )
    work[first : first + TILE, :] = rows
    if first + TILE < K:
        change = lax.dot_general(
            rows[:, 0:128], rows, (((0,), (0,)), ((), ())), precision=HI,
            preferred_element_type=F32,
        )
        work[first + TILE :, :] = work[first + TILE :, :] - change[first + TILE :, :]


def iterate_kernel(packed, start, basis, gram, work):
    unpack(packed[...], gram)
    work[:, K:] = start[...]

    def step(_, carry):
        image = jnp.dot(work[:, K:], gram[...], precision=HI, preferred_element_type=F32)
        work[:, 0:K] = lax.dot_general(
            image, image, (((1,), (1,)), ((), ())), precision=HI, preferred_element_type=F32
        )
        work[:, K:] = image
        for index in range(K // TILE):
            eliminate(work, index)
        return carry

    lax.fori_loop(0, ITERS, step, 0)
    basis[...] = work[:, K:]


def iterate(packed, start):
    return pl.pallas_call(
        iterate_kernel,
        out_shape=jax.ShapeDtypeStruct((K, SPAN), F32),
        in_specs=[VMEM, VMEM],
        out_specs=VMEM,
        scratch_shapes=[pltpu.VMEM((SPAN, SPAN), F32), pltpu.VMEM((K, K + SPAN), F32)],
        cost_estimate=pl.CostEstimate(flops=2 * 10**9, bytes_accessed=10**6, transcendentals=0),
        name="iterate",
    )(packed, start)


def finish_kernel(
    place, low, high, mine, other, frames, tail, near, far, power, basis, proj, chunk
):
    step = pl.program_id(0)
    core = place[0] == 1
    last = place[1] == 1
    half = pl.num_programs(0) // 2

    @pl.when(step == 0)
    def _():
        chunk[...] = jnp.zeros_like(chunk)
        index = grid_of((K, USED), 0)
        for window in range(2):
            own = core if window else jnp.logical_not(core)
            rows = jnp.where(own, mine[...], other[...])
            used = rows[:, 0:USED]
            kept = jnp.where((index >= low[window]) & (index < high[window]), used, 0.0)
            proj[window] = lax.dot_general(
                kept, used, (((0,), (0,)), ((), ())), precision=HI, preferred_element_type=F32
            ).astype(BF16)
            ends = rows[:, 256:384].T
            basis[window, 0:MAIN] = rows[:, 0:128].T
            basis[window, MAIN:HALF] = ends[0:REM]
            basis[window, HALF : HALF + MAIN] = rows[:, 128:256].T
            basis[window, HALF + MAIN : WINDOW] = ends[32 : 32 + REM]

    def fill(at, block):
        chunk[128 * at : 128 * at + MAIN, :] = block[0:MAIN]
        chunk[256 + 32 * at : 256 + 32 * at + REM, :] = block[MAIN:HALF]

    for window in range(2):
        total = jnp.zeros((1, chunk.shape[1]), F32)
        for part in range(2):
            if window == 0:
                one, two = frames[part, 0], frames[part, 1]
            else:
                one = frames[part, 1]
                two = jnp.where(last, tail[part], jnp.where(step < half, near[part], far[part]))
            fill(0, one)
            fill(1, two)
            out = jnp.dot(proj[window], chunk[...], preferred_element_type=F32)
            total += jnp.sum(out * out, axis=0, keepdims=True)
        power[window : window + 1, :] = total / WINDOW


def finish(place, low, high, mine, other, frames, tail, near, far):
    pixels = frames.shape[-1]
    steps = 8
    width = pixels // steps
    turn = steps // 2
    return pl.pallas_call(
        finish_kernel,
        grid=(steps,),
        out_shape=(
            jax.ShapeDtypeStruct((2, pixels), F32),
            jax.ShapeDtypeStruct((2, WINDOW, K), F32),
        ),
        in_specs=[
            SMEM,
            SMEM,
            SMEM,
            pl.BlockSpec((K, SPAN), lambda i: (0, 0)),
            pl.BlockSpec((K, SPAN), lambda i: (0, 0)),
            pl.BlockSpec((2, 2, HALF, width), lambda i: (0, 0, 0, i)),
            pl.BlockSpec((2, HALF, width), lambda i: (0, 0, i)),
            pl.BlockSpec((2, HALF, width), lambda i: (0, 0, jnp.minimum(i, turn - 1))),
            pl.BlockSpec((2, HALF, width), lambda i: (0, 0, jnp.maximum(i - turn, 0))),
        ],
        out_specs=(
            pl.BlockSpec((2, width), lambda i: (0, i)),
            pl.BlockSpec((2, WINDOW, K), lambda i: (0, 0, 0)),
        ),
        scratch_shapes=[pltpu.VMEM((2, USED, USED), BF16), pltpu.VMEM((USED, width), BF16)],
        cost_estimate=pl.CostEstimate(flops=7 * 10**9, bytes_accessed=10**7, transcendentals=0),
        name="finish",
    )(place, low, high, mine, other, frames, tail, near, far)


def in_lanes(start):
    rows = start.T
    gap = jnp.zeros((K, 32 - REM), F32)
    rest = jnp.zeros((K, 64), F32)
    return jnp.concatenate(
        [
            rows[:, 0:MAIN],
            rows[:, HALF : HALF + MAIN],
            rows[:, MAIN:HALF],
            gap,
            rows[:, HALF + MAIN :],
            gap,
            rest,
        ],
        axis=1,
    )


def body(iq, tail_frames, start_basis, low_rank, high_rank):
    pixels = iq.shape[-1]
    half = pixels // 2
    core = lax.axis_index("pix_3")
    block = lax.axis_index("tm")
    place = jnp.stack([core, block]).astype(jnp.int32)
    chips = lax.axis_size(CHIPS)

    sent = jnp.where(block == 1, iq[:HALF, :, :half], iq[HALF:, :, half:])
    near = lax.ppermute(jnp.swapaxes(sent, 0, 1), "tm", [(0, 1), (1, 0)])
    frames = jnp.transpose(iq.reshape(2, HALF, 2, pixels), (2, 0, 1, 3))
    tail = jnp.swapaxes(tail_frames, 0, 1)
    even, odd, extra = local_products(place, frames, tail)
    keep, swap, send = cross_products(place, frames, near, even, odd, extra)
    far = lax.ppermute(frames[:, 0, :, half:], "tm", [(1, 0)])
    swapped = lax.ppermute(swap, "pix_3", [(0, 1), (1, 0)])
    own = lax.ppermute(send, ("pix_3", "tm"), [(3, 2)])
    across_core = lax.ppermute(send, ("pix_3", "tm"), [(1, 2)])
    mine = keep + swapped + own + across_core
    pieces = lax.all_to_all(mine.reshape(chips, PACKED // chips, 128), CHIPS, 0, 0, tiled=True)
    piece = pieces.sum(axis=0)
    packed = lax.all_to_all(
        jnp.broadcast_to(piece[None], pieces.shape), CHIPS, 0, 0, tiled=True
    ).reshape(PACKED, 128)
    found = iterate(packed, in_lanes(start_basis))
    other = lax.ppermute(found, "pix_3", [(0, 1), (1, 0)])
    return finish(place, low_rank, high_rank, found, other, frames, tail, near, far)


def solution(mesh):
    torus = Mesh(
        mesh.devices.reshape(2, 8, 4, 2, mesh.shape["tm"]),
        ("pix_0", "pix_1", "pix_2", "pix_3", "tm"),
    )
    return jax.shard_map(
        body,
        mesh=torus,
        in_specs=(P("tm", None, PIX), P(None, None, PIX), P(), P("tm"), P("tm")),
        out_specs=(P("tm", PIX), P("tm", None, None)),
        check_vma=False,
    )
```

```python
import functools

import jax
import jax.numpy as jnp
from jax import lax
from jax.experimental import pallas as pl
from jax.experimental.pallas import tpu as pltpu
from jax.sharding import Mesh
from jax.sharding import PartitionSpec as P

K = 128
ITERS = 3
WINDOW = 300
HALF = 150
MAIN = 128
REM = HALF - MAIN
SPAN = 384
USED = 320
TILE = 32
PACKED = 512
EXTRA = 288
LATE = 184
CHUNK = 512
LIMIT = 20 * 2**20
HI = lax.Precision.HIGHEST
F32 = jnp.float32
BF16 = jnp.bfloat16
PIX = ("pix_0", "pix_1", "pix_2", "pix_3")
CHIPS = ("pix_0", "pix_1", "pix_2")
SMEM = pl.BlockSpec(memory_space=pltpu.SMEM)
VMEM = pl.BlockSpec(memory_space=pltpu.VMEM)


def grid_of(shape, axis):
    return lax.broadcasted_iota(jnp.int32, shape, axis)


def across(a, b):
    return lax.dot_general(a, b, (((1,), (1,)), ((), ())), preferred_element_type=F32)


def parameters():
    return pltpu.CompilerParams(vmem_limit_bytes=LIMIT)


def pick_kernel(place, source, out, done):
    first = 1 - place[1]
    width = out.shape[-1]
    copy = pltpu.make_async_copy(
        source.at[
            pl.ds(first * HALF, HALF), :, pl.ds(pl.multiple_of(first * width, 128), width)
        ],
        out,
        done,
    )
    copy.start()
    copy.wait()


def picked(place, iq):
    half = iq.shape[-1] // 2
    return pl.pallas_call(
        pick_kernel,
        out_shape=jax.ShapeDtypeStruct((HALF, 2, half), iq.dtype),
        in_specs=[SMEM, pl.BlockSpec(memory_space=pltpu.HBM)],
        out_specs=VMEM,
        scratch_shapes=[pltpu.SemaphoreType.DMA],
        name="picked",
    )(place, iq)


def lower_and_diagonal(block):
    row = grid_of((MAIN, 128), 0)
    lane = grid_of((MAIN, 128), 1)
    diagonal = jnp.where(
        grid_of((8, 128), 0) == 0,
        jnp.sum(jnp.where(lane == row, block, 0.0), axis=0, keepdims=True),
        0.0,
    )
    return jnp.where(lane < row, block, 0.0), diagonal


def packed_rows(first, cross, second):
    row = grid_of((MAIN, 128), 0)
    lane = grid_of((MAIN, 128), 1)
    lower, diagonal = lower_and_diagonal(second[0:MAIN, 0:128])
    corner = jnp.where(lane >= row, first[0:MAIN, 0:128], lower)
    side = (
        first[0:152, 128:256]
        + pltpu.roll(cross[0:152, 128:256], 32, 1)
        + pltpu.roll(second[0:152, 128:256], 64, 1)
    )
    return corner, cross[0:152, 0:128], side, diagonal


def local_kernel(place, frames, tail, keep, swap, extra, mine, sums):
    sums[...] = jnp.zeros_like(sums)
    width = 1024
    half = mine.shape[-1]
    part_of = pl.ds(pl.multiple_of(place[1] * half, 128), half)
    for part in range(2):
        mine[part] = frames[part, 1 - place[1], :, part_of]

    def step(i, carry):
        at = pl.ds(pl.multiple_of(i * width, 128), width)
        for part in range(2):
            a = frames[part, 0, :, at]
            b = frames[part, 1, :, at]
            c = tail[part, :, at]
            for index, (left, right) in enumerate(((a, a), (a, b), (b, b), (b, c), (c, c))):
                sums[index, 0:HALF, 0:HALF] += across(left, right)
        return carry

    lax.fori_loop(0, frames.shape[-1] // width, step, 0)
    core = place[0] == 1
    scale = place[1].astype(F32)
    even = packed_rows(sums[0], sums[1], sums[2])
    odd = packed_rows(sums[2], sums[3] * scale, sums[4] * scale)
    at = 0
    for one, two in zip(even, odd):
        rows = one.shape[0]
        keep[at : at + rows] = jnp.where(core, two, one)
        swap[at : at + rows] = jnp.where(core, one, two)
        at += rows
    keep[440:] = jnp.zeros((PACKED - 440, 128), F32)
    swap[440:] = jnp.zeros((PACKED - 440, 128), F32)
    lower, diagonal = lower_and_diagonal(sums[0, 0:MAIN, 0:128])
    extra[0:MAIN] = lower
    extra[MAIN : MAIN + 152] = pltpu.roll(sums[0, 0:152, 128:256], 64, 1)
    extra[MAIN + 152 : EXTRA] = diagonal


def local_products(place, frames, tail):
    shape = jax.ShapeDtypeStruct((PACKED, 128), F32)
    return pl.pallas_call(
        local_kernel,
        out_shape=(
            shape,
            shape,
            jax.ShapeDtypeStruct((EXTRA, 128), F32),
            jax.ShapeDtypeStruct((2, HALF, frames.shape[-1] // 2), BF16),
        ),
        in_specs=[SMEM, VMEM, VMEM],
        out_specs=(VMEM, VMEM, VMEM, VMEM),
        scratch_shapes=[pltpu.VMEM((5, 152, 256), F32)],
        cost_estimate=pl.CostEstimate(flops=4 * 10**9, bytes_accessed=8 * 10**6, transcendentals=0),
        compiler_params=parameters(),
        name="local_products",
    )(place, frames, tail)


def cross_kernel(place, own, arrived, late, sums):
    total = jnp.zeros((HALF, HALF), F32)
    for part in range(2):
        total += across(own[part], arrived[part])
    sums[...] = jnp.zeros_like(sums)
    sums[0:HALF, 0:HALF] = total

    @pl.when(place[1] == 1)
    def _():
        sums[0:256] = sums[...].T

    late[0:152] = sums[0:152, 0:128]
    side = jnp.zeros((32, 128), F32)
    for g in range(5):
        rows = sums[32 * g : 32 * g + 32, 128:256]
        side += pltpu.roll(rows, 24 * g, 1) if g else rows
    late[152:LATE] = side


def cross_products(place, own, arrived):
    return pl.pallas_call(
        cross_kernel,
        out_shape=jax.ShapeDtypeStruct((LATE, 128), F32),
        in_specs=[SMEM, VMEM, VMEM],
        out_specs=VMEM,
        scratch_shapes=[pltpu.VMEM((256, 256), F32)],
        cost_estimate=pl.CostEstimate(flops=4 * 10**8, bytes_accessed=3 * 10**6, transcendentals=0),
        compiler_params=parameters(),
        name="cross_products",
    )(place, own, arrived)


def merge_kernel(place, keep, swapped, extra_one, extra_two, own, one, two, three, out):
    out[...] = keep[...] + swapped[...]
    extra = extra_one[...] + extra_two[...]
    out[0:MAIN] += extra[0:MAIN]
    out[280:440] += extra[MAIN:EXTRA]

    @pl.when((place[0] == 1) & (place[1] == 0))
    def _():
        late = own[...] + one[...] + two[...] + three[...]
        out[128:280] += late[0:152]
        lane = grid_of((32, 128), 1)
        valid = (lane >= 32) & (lane < 56)
        for g in range(5):
            rows = 24 if g == 4 else 32
            moved = jnp.where(valid, pltpu.roll(late[152:LATE], (32 - 24 * g) % 128, 1), 0.0)
            out[280 + 32 * g : 280 + 32 * g + rows] += moved[0:rows]


def merged(place, *parts):
    return pl.pallas_call(
        merge_kernel,
        out_shape=jax.ShapeDtypeStruct((PACKED, 128), F32),
        in_specs=[SMEM] + [VMEM] * len(parts),
        out_specs=VMEM,
        compiler_params=parameters(),
        name="merged",
    )(place, *parts)


def unpack(rows, gram):
    row = grid_of((128, 128), 0)
    lane = grid_of((128, 128), 1)
    both = rows[0:128]
    turned = both.T
    gram[0:128, 0:128] = jnp.where(lane >= row, both, turned)
    gram[128:256, 128:256] = jnp.where(
        lane < row, both, jnp.where(lane == row, rows[432:433], turned)
    )
    cross = rows[128:256]
    gram[0:128, 128:256] = cross
    gram[128:256, 0:128] = cross.T
    side = rows[280:408]
    turn = jnp.concatenate([rows[256:280], jnp.zeros((104, 128), F32)], axis=0).T
    first = jnp.where(lane < 64, side, 0.0)
    second = jnp.where(lane < 32, turn, jnp.where(lane < 64, pltpu.roll(side, 96, 1), 0.0))
    gram[0:128, 256:384] = first
    gram[128:256, 256:384] = second
    gram[256:384, 0:128] = first.T
    gram[256:384, 128:256] = second.T
    corner = rows[408:432]
    gram[256:384, 256:384] = jnp.zeros((128, 128), F32)
    short = grid_of((24, 128), 1)
    gram[256:280, 256:384] = jnp.where(short < 64, corner, 0.0)
    moved = pltpu.roll(corner, 96, 1)
    square = jnp.concatenate(
        [jnp.where(short < 32, moved, 0.0), jnp.zeros((104, 128), F32)], axis=0
    ).T[0:24]
    gram[288:312, 256:384] = jnp.where(
        short < 32, square, jnp.where(short < 64, moved, 0.0)
    )


def row_of(vector, index):
    return jnp.broadcast_to(vector[index : index + 1, :], vector.shape)


def eliminate(work, step):
    first = TILE * step
    sub = grid_of((8, 128), 0)
    lane = grid_of((8, 128), 1)
    groups = TILE // 8
    cols = {}
    for g in range(groups):
        top = first + 8 * g
        block = work[top : top + 8, 0:128]
        for k in range(8 * (g + 1)):
            at = first + k
            cols[g, k] = jnp.broadcast_to(block[:, at : at + 1], (8, 128))
    inverse = [jnp.where(lane == sub + 8 * g, 1.0, 0.0).astype(F32) for g in range(groups)]
    for j in range(TILE):
        gj, rj = divmod(j, 8)
        scale = lax.rsqrt(row_of(cols[gj, j], rj))
        for g in range(gj, groups):
            cols[g, j] = cols[g, j] * scale
        for k in range(j + 1, TILE):
            gk, rk = divmod(k, 8)
            factor = row_of(cols[gk, j], rk)
            for g in range(gk, groups):
                cols[g, k] = cols[g, k] - cols[g, j] * factor
        pivot = row_of(inverse[gj], rj) * scale
        for g in range(gj, groups):
            if g == gj:
                below = jnp.where(sub > rj, cols[g, j], 0.0)
                inverse[g] = jnp.where(sub == rj, pivot, inverse[g] - below * pivot)
            else:
                inverse[g] = inverse[g] - cols[g, j] * pivot
    lhs = jnp.concatenate(inverse, axis=0)[:, 0:TILE]
    rows = jnp.dot(
        lhs, work[first : first + TILE, :], precision=HI, preferred_element_type=F32
    )
    work[first : first + TILE, :] = rows
    if first + TILE < K:
        change = lax.dot_general(
            rows[:, 0:128], rows, (((0,), (0,)), ((), ())), precision=HI,
            preferred_element_type=F32,
        )
        work[first + TILE :, :] = work[first + TILE :, :] - change[first + TILE :, :]


def iterate_kernel(packed, start, basis, gram, work):
    unpack(packed[...], gram)
    work[:, K:] = start[...]

    def step(_, carry):
        image = jnp.dot(work[:, K:], gram[...], precision=HI, preferred_element_type=F32)
        work[:, 0:K] = lax.dot_general(
            image, image, (((1,), (1,)), ((), ())), precision=HI, preferred_element_type=F32
        )
        work[:, K:] = image
        for index in range(K // TILE):
            eliminate(work, index)
        return carry

    lax.fori_loop(0, ITERS, step, 0)
    basis[...] = work[:, K:]


def iterate(packed, start):
    return pl.pallas_call(
        iterate_kernel,
        out_shape=jax.ShapeDtypeStruct((K, SPAN), F32),
        in_specs=[VMEM, VMEM],
        out_specs=VMEM,
        scratch_shapes=[pltpu.VMEM((SPAN, SPAN), F32), pltpu.VMEM((K, K + SPAN), F32)],
        cost_estimate=pl.CostEstimate(flops=2 * 10**9, bytes_accessed=10**6, transcendentals=0),
        compiler_params=pltpu.CompilerParams(vmem_limit_bytes=LIMIT),
        name="iterate",
    )(packed, start)


def projection(rows, low, high):
    used = rows[:, 0:USED]
    index = grid_of((K, USED), 0)
    kept = jnp.where((index >= low) & (index < high), used, 0.0)
    return lax.dot_general(
        kept, used, (((0,), (0,)), ((), ())), precision=HI, preferred_element_type=F32
    ).astype(BF16)


def powers(proj, chunk, power, first, second, begin, pixels):
    def step(i, carry):
        at = i * CHUNK
        total = jnp.zeros((1, CHUNK), F32)
        for part in range(2):
            for side, (ref, index, offset) in enumerate((first, second)):
                where = pl.ds(pl.multiple_of(offset + at, 128), CHUNK)
                block = ref[part, :, where] if index is None else ref[part, index, :, where]
                chunk[part, 128 * side : 128 * side + MAIN, :] = block[0:MAIN]
                chunk[part, 256 + 32 * side : 256 + 32 * side + REM, :] = block[MAIN:HALF]
            out = jnp.dot(proj[...], chunk[part], preferred_element_type=F32)
            total += jnp.sum(out * out, axis=0, keepdims=True)
        power[:, pl.ds(pl.multiple_of(begin + at, 128), CHUNK)] = total / WINDOW
        return carry

    lax.fori_loop(0, pixels // CHUNK, step, 0, unroll=2)


def whole_window(place, proj, chunk, power, frames, tail, odd):
    pixels = frames.shape[-1]

    @pl.when(jnp.logical_not(odd))
    def _():
        powers(proj, chunk, power, (frames, 0, 0), (frames, 1, 0), 0, pixels)

    @pl.when(odd & (place[1] == 1))
    def _():
        powers(proj, chunk, power, (frames, 1, 0), (tail, None, 0), 0, pixels)


def own_kernel(place, low, high, mine, frames, tail, power, proj, chunk):
    chunk[...] = jnp.zeros_like(chunk)
    which = place[0]
    proj[...] = projection(mine[...], low[which], high[which])
    whole_window(place, proj, chunk, power, frames, tail, which == 1)


def shared_kernel(place, low, high, mine, other, one, two, frames, near, power, proj, chunk):
    chunk[...] = jnp.zeros_like(chunk)
    pixels = near.shape[-1]
    last = place[1] == 1
    found = jnp.where(
        last, one[...] + two[...], jnp.where(place[0] == 1, mine[...], other[...])
    )
    proj[...] = projection(found, low[2], high[2])

    @pl.when(last)
    def _():
        powers(proj, chunk, power, (near, None, 0), (frames, 0, pixels), 0, pixels)

    @pl.when(jnp.logical_not(last))
    def _():
        powers(proj, chunk, power, (frames, 1, 0), (near, None, 0), 0, pixels)


def other_kernel(place, low, high, mine, other, frames, tail, power, basis, proj, chunk):
    chunk[...] = jnp.zeros_like(chunk)
    which = 1 - place[0]
    proj[...] = projection(other[...], low[which], high[which])
    whole_window(place, proj, chunk, power, frames, tail, which == 1)
    core = place[0] == 1
    for window in range(2):
        own = core if window else jnp.logical_not(core)
        rows = jnp.where(own, mine[...], other[...])
        ends = rows[:, 256:384].T
        basis[0:MAIN, window, :] = rows[:, 0:128].T
        basis[MAIN:HALF, window, :] = ends[0:REM]
        basis[HALF : HALF + MAIN, window, :] = rows[:, 128:256].T
        basis[HALF + MAIN : WINDOW, window, :] = ends[32 : 32 + REM]


def power_call(kernel, name, pixels, flops, with_basis, *arrays):
    shape = jax.ShapeDtypeStruct((1, pixels), F32)
    return pl.pallas_call(
        kernel,
        out_shape=(shape, jax.ShapeDtypeStruct((WINDOW, 2, K), F32)) if with_basis else shape,
        in_specs=[SMEM] * 3 + [VMEM] * (len(arrays) - 3),
        out_specs=(VMEM, VMEM) if with_basis else VMEM,
        scratch_shapes=[pltpu.VMEM((USED, USED), BF16), pltpu.VMEM((2, USED, CHUNK), BF16)],
        cost_estimate=pl.CostEstimate(flops=flops, bytes_accessed=10**7, transcendentals=0),
        compiler_params=parameters(),
        name=name,
    )(*arrays)


def in_lanes(start):
    rows = start.T
    gap = jnp.zeros((K, 32 - REM), F32)
    rest = jnp.zeros((K, 64), F32)
    return jnp.concatenate(
        [
            rows[:, 0:MAIN],
            rows[:, HALF : HALF + MAIN],
            rows[:, MAIN:HALF],
            gap,
            rows[:, HALF + MAIN :],
            gap,
            rest,
        ],
        axis=1,
    )


def body(iq, tail_frames, start_basis, low_rank, high_rank):
    pixels = iq.shape[-1]
    half = pixels // 2
    core = lax.axis_index("pix_3")
    block = lax.axis_index("tm")
    place = jnp.stack([core, block]).astype(jnp.int32)
    chips = lax.axis_size(CHIPS)
    pair = ("pix_3", "tm")

    near = lax.ppermute(picked(place, iq), "tm", [(0, 1), (1, 0)])
    frames = jnp.transpose(iq.reshape(2, HALF, 2, pixels), (2, 0, 1, 3))
    tail = jnp.swapaxes(tail_frames, 0, 1)
    keep, swap, extra, own_half = local_products(place, frames, tail)
    swapped = lax.ppermute(swap, "pix_3", [(0, 1), (1, 0)])
    extra_one = lax.ppermute(extra, pair, [(3, 2)])
    extra_two = lax.ppermute(extra, pair, [(1, 2)])
    near = jnp.swapaxes(near, 0, 1)
    late = cross_products(place, own_half, near)
    one = lax.ppermute(late, pair, [(3, 2)])
    two = lax.ppermute(late, pair, [(1, 2)])
    three = lax.ppermute(late, pair, [(0, 2)])
    mine = merged(place, keep, swapped, extra_one, extra_two, late, one, two, three)
    pieces = lax.all_to_all(mine.reshape(chips, PACKED // chips, 128), CHIPS, 0, 0, tiled=True)
    piece = pieces.sum(axis=0)
    packed = lax.all_to_all(
        jnp.broadcast_to(piece[None], pieces.shape), CHIPS, 0, 0, tiled=True
    ).reshape(PACKED, 128)
    found = iterate(packed, in_lanes(start_basis))
    one = lax.ppermute(found, pair, [(2, 3)])
    two = lax.ppermute(found, pair, [(2, 1)])
    other = lax.ppermute(found, "pix_3", [(0, 1), (1, 0)])
    lows = jnp.concatenate([low_rank, lax.ppermute(low_rank[1:], "tm", [(0, 1)])])
    highs = jnp.concatenate([high_rank, lax.ppermute(high_rank[1:], "tm", [(0, 1)])])
    lows = jnp.where(block == 0, jnp.concatenate([low_rank, low_rank[1:]]), lows)
    highs = jnp.where(block == 0, jnp.concatenate([high_rank, high_rank[1:]]), highs)
    flops = 3 * 10**9
    own = power_call(
        own_kernel, "own", pixels, flops, False, place, lows, highs, found, frames, tail
    )
    shared = power_call(
        shared_kernel, "shared", half, flops // 2, False,
        place, lows, highs, found, other, one, two, frames, near,
    )
    back = lax.ppermute(shared, "tm", [(1, 0)])
    rest, basis = power_call(
        other_kernel, "other", pixels, flops, True,
        place, lows, highs, found, other, frames, tail,
    )
    even = jnp.where(core == 0, own, rest)
    odd = jnp.where(core == 0, rest, own)
    odd = jnp.where(block == 0, jnp.concatenate([shared, back], axis=1), odd)
    return jnp.concatenate([even, odd], axis=0), jnp.swapaxes(basis, 0, 1)


def solution(mesh):
    torus = Mesh(
        mesh.devices.reshape(2, 8, 4, 2, mesh.shape["tm"]),
        ("pix_0", "pix_1", "pix_2", "pix_3", "tm"),
    )
    return jax.shard_map(
        body,
        mesh=torus,
        in_specs=(P("tm", None, PIX), P(None, None, PIX), P(), P("tm"), P("tm")),
        out_specs=(P("tm", PIX), P("tm", None, None)),
        check_vma=False,
    )
```

```python
import functools

import jax
import jax.numpy as jnp
from jax import lax
from jax.experimental import pallas as pl
from jax.experimental.pallas import tpu as pltpu
from jax.sharding import Mesh
from jax.sharding import PartitionSpec as P

K = 128
ITERS = 3
WINDOW = 300
HALF = 150
MAIN = 128
REM = HALF - MAIN
SPAN = 384
USED = 320
FLAG = 320
TILE = 32
PACKED = 512
EXTRA = 288
LATE = 184
CHUNK = 1024
LIMIT = 20 * 2**20
HI = lax.Precision.HIGHEST
F32 = jnp.float32
BF16 = jnp.bfloat16
PIX = ("pix_0", "pix_1", "pix_2", "pix_3")
PLANE = ("pix_1", "pix_2")
SMEM = pl.BlockSpec(memory_space=pltpu.SMEM)
VMEM = pl.BlockSpec(memory_space=pltpu.VMEM)


def grid_of(shape, axis):
    return lax.broadcasted_iota(jnp.int32, shape, axis)


def across(a, b):
    return lax.dot_general(a, b, (((1,), (1,)), ((), ())), preferred_element_type=F32)


def parameters():
    return pltpu.CompilerParams(vmem_limit_bytes=LIMIT)


def pick_kernel(place, source, out, done):
    first = 1 - place[1]
    width = out.shape[-1]
    copy = pltpu.make_async_copy(
        source.at[
            pl.ds(first * HALF, HALF), :, pl.ds(pl.multiple_of(first * width, 128), width)
        ],
        out,
        done,
    )
    copy.start()
    copy.wait()


def picked(place, iq):
    half = iq.shape[-1] // 2
    return pl.pallas_call(
        pick_kernel,
        out_shape=jax.ShapeDtypeStruct((HALF, 2, half), iq.dtype),
        in_specs=[SMEM, pl.BlockSpec(memory_space=pltpu.HBM)],
        out_specs=VMEM,
        scratch_shapes=[pltpu.SemaphoreType.DMA],
        name="picked",
    )(place, iq)


def lower_and_diagonal(block):
    row = grid_of((MAIN, 128), 0)
    lane = grid_of((MAIN, 128), 1)
    diagonal = jnp.where(
        grid_of((8, 128), 0) == 0,
        jnp.sum(jnp.where(lane == row, block, 0.0), axis=0, keepdims=True),
        0.0,
    )
    return jnp.where(lane < row, block, 0.0), diagonal


def packed_rows(first, cross, second):
    row = grid_of((MAIN, 128), 0)
    lane = grid_of((MAIN, 128), 1)
    lower, diagonal = lower_and_diagonal(second[0:MAIN, 0:128])
    corner = jnp.where(lane >= row, first[0:MAIN, 0:128], lower)
    side = (
        first[0:152, 128:256]
        + pltpu.roll(cross[0:152, 128:256], 32, 1)
        + pltpu.roll(second[0:152, 128:256], 64, 1)
    )
    return corner, cross[0:152, 0:128], side, diagonal


def local_kernel(place, frames, tail, keep, swap, extra, mine, sums):
    sums[...] = jnp.zeros_like(sums)
    width = 1024
    half = mine.shape[-1]
    part_of = pl.ds(pl.multiple_of(place[1] * half, 128), half)
    for part in range(2):
        mine[part] = frames[part, 1 - place[1], :, part_of]

    def step(i, carry):
        at = pl.ds(pl.multiple_of(i * width, 128), width)
        for part in range(2):
            a = frames[part, 0, :, at]
            b = frames[part, 1, :, at]
            c = tail[part, :, at]
            for index, (left, right) in enumerate(((a, a), (a, b), (b, b), (b, c), (c, c))):
                sums[index, 0:HALF, 0:HALF] += across(left, right)
        return carry

    lax.fori_loop(0, frames.shape[-1] // width, step, 0)
    core = place[0] == 1
    scale = place[1].astype(F32)
    even = packed_rows(sums[0], sums[1], sums[2])
    odd = packed_rows(sums[2], sums[3] * scale, sums[4] * scale)
    at = 0
    for one, two in zip(even, odd):
        rows = one.shape[0]
        keep[at : at + rows] = jnp.where(core, two, one)
        swap[at : at + rows] = jnp.where(core, one, two)
        at += rows
    keep[440:] = jnp.zeros((PACKED - 440, 128), F32)
    swap[440:] = jnp.zeros((PACKED - 440, 128), F32)
    lower, diagonal = lower_and_diagonal(sums[0, 0:MAIN, 0:128])
    extra[0:MAIN] = lower
    extra[MAIN : MAIN + 152] = pltpu.roll(sums[0, 0:152, 128:256], 64, 1)
    extra[MAIN + 152 : EXTRA] = diagonal


def local_products(place, frames, tail):
    shape = jax.ShapeDtypeStruct((PACKED, 128), F32)
    return pl.pallas_call(
        local_kernel,
        out_shape=(
            shape,
            shape,
            jax.ShapeDtypeStruct((EXTRA, 128), F32),
            jax.ShapeDtypeStruct((2, HALF, frames.shape[-1] // 2), BF16),
        ),
        in_specs=[SMEM, VMEM, VMEM],
        out_specs=(VMEM, VMEM, VMEM, VMEM),
        scratch_shapes=[pltpu.VMEM((5, 152, 256), F32)],
        cost_estimate=pl.CostEstimate(flops=4 * 10**9, bytes_accessed=8 * 10**6, transcendentals=0),
        compiler_params=parameters(),
        name="local_products",
    )(place, frames, tail)


def cross_kernel(place, own, arrived, late, sums):
    total = jnp.zeros((HALF, HALF), F32)
    for part in range(2):
        total += across(own[part], arrived[part])
    sums[...] = jnp.zeros_like(sums)
    sums[0:HALF, 0:HALF] = total

    @pl.when(place[1] == 1)
    def _():
        sums[0:256] = sums[...].T

    late[0:152] = sums[0:152, 0:128]
    side = jnp.zeros((32, 128), F32)
    for g in range(5):
        rows = sums[32 * g : 32 * g + 32, 128:256]
        side += pltpu.roll(rows, 24 * g, 1) if g else rows
    late[152:LATE] = side


def cross_products(place, own, arrived):
    return pl.pallas_call(
        cross_kernel,
        out_shape=jax.ShapeDtypeStruct((LATE, 128), F32),
        in_specs=[SMEM, VMEM, VMEM],
        out_specs=VMEM,
        scratch_shapes=[pltpu.VMEM((256, 256), F32)],
        cost_estimate=pl.CostEstimate(flops=4 * 10**8, bytes_accessed=3 * 10**6, transcendentals=0),
        compiler_params=parameters(),
        name="cross_products",
    )(place, own, arrived)


def merge_kernel(place, keep, swapped, extra_one, extra_two, own, one, two, three, out):
    out[...] = keep[...] + swapped[...]
    extra = extra_one[...] + extra_two[...]
    out[0:MAIN] += extra[0:MAIN]
    out[280:440] += extra[MAIN:EXTRA]

    @pl.when((place[0] == 1) & (place[1] == 0))
    def _():
        late = own[...] + one[...] + two[...] + three[...]
        out[128:280] += late[0:152]
        lane = grid_of((32, 128), 1)
        valid = (lane >= 32) & (lane < 56)
        for g in range(5):
            rows = 24 if g == 4 else 32
            moved = jnp.where(valid, pltpu.roll(late[152:LATE], (32 - 24 * g) % 128, 1), 0.0)
            out[280 + 32 * g : 280 + 32 * g + rows] += moved[0:rows]


def merged(place, *parts):
    return pl.pallas_call(
        merge_kernel,
        out_shape=jax.ShapeDtypeStruct((PACKED, 128), F32),
        in_specs=[SMEM] + [VMEM] * len(parts),
        out_specs=VMEM,
        compiler_params=parameters(),
        name="merged",
    )(place, *parts)


def unpack(rows, gram):
    row = grid_of((128, 128), 0)
    lane = grid_of((128, 128), 1)
    both = rows[0:128]
    turned = both.T
    gram[0:128, 0:128] = jnp.where(lane >= row, both, turned)
    gram[128:256, 128:256] = jnp.where(
        lane < row, both, jnp.where(lane == row, rows[432:433], turned)
    )
    cross = rows[128:256]
    gram[0:128, 128:256] = cross
    gram[128:256, 0:128] = cross.T
    side = rows[280:408]
    turn = jnp.concatenate([rows[256:280], jnp.zeros((104, 128), F32)], axis=0).T
    first = jnp.where(lane < 64, side, 0.0)
    second = jnp.where(lane < 32, turn, jnp.where(lane < 64, pltpu.roll(side, 96, 1), 0.0))
    gram[0:128, 256:384] = first
    gram[128:256, 256:384] = second
    gram[256:384, 0:128] = first.T
    gram[256:384, 128:256] = second.T
    corner = rows[408:432]
    gram[256:384, 256:384] = jnp.zeros((128, 128), F32)
    short = grid_of((24, 128), 1)
    gram[256:280, 256:384] = jnp.where(short < 64, corner, 0.0)
    moved = pltpu.roll(corner, 96, 1)
    square = jnp.concatenate(
        [jnp.where(short < 32, moved, 0.0), jnp.zeros((104, 128), F32)], axis=0
    ).T[0:24]
    gram[288:312, 256:384] = jnp.where(
        short < 32, square, jnp.where(short < 64, moved, 0.0)
    )


def row_of(vector, index):
    return jnp.broadcast_to(vector[index : index + 1, :], vector.shape)


def thirds(x):
    one = x.astype(BF16)
    rest = x - one.astype(F32)
    two = rest.astype(BF16)
    return one, two, (rest - two.astype(F32)).astype(BF16)


def wide_first(x):
    one, two, three = thirds(x)
    group = grid_of(x.shape, 1) // TILE
    head = jnp.where(group == 2, two.astype(F32), one.astype(F32)).astype(BF16)
    tail = jnp.where(
        group == 0, two.astype(F32), jnp.where(group == 1, three.astype(F32), 0.0)
    ).astype(BF16)
    return jnp.concatenate([head, tail], axis=1)


def wide_second(x):
    one, two, three = thirds(x)
    group = grid_of(x.shape, 1) // TILE
    head = jnp.where(
        group == 1, two.astype(F32), jnp.where(group == 3, three.astype(F32), one.astype(F32))
    ).astype(BF16)
    tail = jnp.where(
        group == 0, two.astype(F32), jnp.where(group == 1, one.astype(F32), 0.0)
    ).astype(BF16)
    return jnp.concatenate([head, tail], axis=1)


def tall_second(x):
    one, two, three = thirds(x)
    zero = jnp.zeros((2 * TILE, x.shape[1]), BF16)
    return jnp.concatenate([one, two, one, three, two, one, zero], axis=0)


def eliminate(work, step):
    first = TILE * step
    left = first + TILE
    sub = grid_of((8, 128), 0)
    lane = grid_of((8, 128), 1)
    groups = TILE // 8
    cols = {}
    for g in range(groups):
        top = first + 8 * g
        block = work[top : top + 8, 0:128]
        for k in range(8 * (g + 1)):
            at = first + k
            cols[g, k] = jnp.broadcast_to(block[:, at : at + 1], (8, 128))
    if left < K:
        below = work[left:, 0:128]
        group = grid_of(below.shape, 1) // TILE
        repeated = jnp.zeros_like(below)
        for c in range(4):
            shift = (TILE * (c - step)) % 128
            moved = pltpu.roll(below, shift, 1) if shift else below
            repeated = jnp.where(group == c, moved, repeated)
        under = wide_first(repeated)
    inverse = [
        jnp.where(lane % TILE == sub + 8 * g, 1.0, 0.0).astype(F32) for g in range(groups)
    ]
    for j in range(TILE):
        gj, rj = divmod(j, 8)
        scale = lax.rsqrt(row_of(cols[gj, j], rj))
        for g in range(gj, groups):
            cols[g, j] = cols[g, j] * scale
        for k in range(j + 1, TILE):
            gk, rk = divmod(k, 8)
            factor = row_of(cols[gk, j], rk)
            for g in range(gk, groups):
                cols[g, k] = cols[g, k] - cols[g, j] * factor
        pivot = row_of(inverse[gj], rj) * scale
        for g in range(gj, groups):
            if g == gj:
                below_pivot = jnp.where(sub > rj, cols[g, j], 0.0)
                inverse[g] = jnp.where(sub == rj, pivot, inverse[g] - below_pivot * pivot)
            else:
                inverse[g] = inverse[g] - cols[g, j] * pivot
    turn = jnp.concatenate(inverse, axis=0)
    rows = jnp.dot(
        wide_first(turn), tall_second(work[first:left, :]), preferred_element_type=F32
    )
    work[first:left, :] = rows
    if left < K:
        tall = wide_second(turn)
        factors = across(under, jnp.concatenate([tall] * 4, axis=0))
        work[left:, :] = work[left:, :] - jnp.dot(
            wide_first(factors), tall_second(rows), preferred_element_type=F32
        )


def iterate_kernel(place, low, high, packed, start, basis, gram, work):
    unpack(packed[...], gram)
    work[:, K:] = start[...]

    def step(_, carry):
        image = jnp.dot(work[:, K:], gram[...], precision=HI, preferred_element_type=F32)
        work[:, 0:K] = lax.dot_general(
            image, image, (((1,), (1,)), ((), ())), precision=HI, preferred_element_type=F32
        )
        work[:, K:] = image
        for index in range(K // TILE):
            eliminate(work, index)
        return carry

    lax.fori_loop(0, ITERS, step, 0)
    which = place[0]
    index = grid_of((K, 128), 0)
    kept = (index >= low[which]) & (index < high[which])
    basis[:, 0:256] = work[:, K : K + 256]
    basis[:, 256:384] = jnp.where(
        grid_of((K, 128), 1) == FLAG - 256, jnp.where(kept, 1.0, 0.0), work[:, K + 256 :]
    )


def iterate(place, low, high, packed, start):
    return pl.pallas_call(
        iterate_kernel,
        out_shape=jax.ShapeDtypeStruct((K, SPAN), F32),
        in_specs=[SMEM, SMEM, SMEM, VMEM, VMEM],
        out_specs=VMEM,
        scratch_shapes=[pltpu.VMEM((SPAN, SPAN), F32), pltpu.VMEM((K, K + SPAN), F32)],
        cost_estimate=pl.CostEstimate(flops=2 * 10**9, bytes_accessed=10**6, transcendentals=0),
        compiler_params=pltpu.CompilerParams(vmem_limit_bytes=LIMIT),
        name="iterate",
    )(place, low, high, packed, start)


def projection(rows):
    used = rows[:, 0:USED]
    kept = used * rows[:, FLAG : FLAG + 1]
    return lax.dot_general(
        kept, used, (((0,), (0,)), ((), ())), precision=HI, preferred_element_type=F32
    ).astype(BF16)


def powers(proj, chunk, power, first, second, begin, pixels):
    def step(i, carry):
        at = i * CHUNK
        total = jnp.zeros((1, CHUNK), F32)
        for part in range(2):
            for side, (ref, index, offset) in enumerate((first, second)):
                where = pl.ds(pl.multiple_of(offset + at, 128), CHUNK)
                block = ref[part, :, where] if index is None else ref[part, index, :, where]
                chunk[part, 128 * side : 128 * side + MAIN, :] = block[0:MAIN]
                chunk[part, 256 + 32 * side : 256 + 32 * side + REM, :] = block[MAIN:HALF]
            out = jnp.dot(proj[...], chunk[part], preferred_element_type=F32)
            total += jnp.sum(out * out, axis=0, keepdims=True)
        power[:, pl.ds(pl.multiple_of(begin + at, 128), CHUNK)] = total / WINDOW
        return carry

    lax.fori_loop(0, pixels // CHUNK, step, 0, unroll=2)


def whole_window(place, proj, chunk, power, frames, tail, odd):
    pixels = frames.shape[-1]

    @pl.when(jnp.logical_not(odd))
    def _():
        powers(proj, chunk, power, (frames, 0, 0), (frames, 1, 0), 0, pixels)

    @pl.when(odd & (place[1] == 1))
    def _():
        powers(proj, chunk, power, (frames, 1, 0), (tail, None, 0), 0, pixels)


def own_kernel(place, mine, frames, tail, power, proj, chunk):
    chunk[...] = jnp.zeros_like(chunk)
    proj[...] = projection(mine[...])
    whole_window(place, proj, chunk, power, frames, tail, place[0] == 1)


def shared_kernel(place, mine, other, one, two, frames, near, power, proj, chunk):
    chunk[...] = jnp.zeros_like(chunk)
    pixels = near.shape[-1]
    last = place[1] == 1
    found = jnp.where(
        last, one[...] + two[...], jnp.where(place[0] == 1, mine[...], other[...])
    )
    proj[...] = projection(found)

    @pl.when(last)
    def _():
        powers(proj, chunk, power, (near, None, 0), (frames, 0, pixels), 0, pixels)

    @pl.when(jnp.logical_not(last))
    def _():
        powers(proj, chunk, power, (frames, 1, 0), (near, None, 0), 0, pixels)


def other_kernel(place, mine, other, frames, tail, power, basis, proj, chunk):
    chunk[...] = jnp.zeros_like(chunk)
    proj[...] = projection(other[...])
    whole_window(place, proj, chunk, power, frames, tail, place[0] == 0)
    core = place[0] == 1
    for window in range(2):
        own = core if window else jnp.logical_not(core)
        rows = jnp.where(own, mine[...], other[...])
        ends = rows[:, 256:384].T
        basis[0:MAIN, window, :] = rows[:, 0:128].T
        basis[MAIN:HALF, window, :] = ends[0:REM]
        basis[HALF : HALF + MAIN, window, :] = rows[:, 128:256].T
        basis[HALF + MAIN : WINDOW, window, :] = ends[32 : 32 + REM]


def power_call(kernel, name, pixels, flops, with_basis, *arrays):
    shape = jax.ShapeDtypeStruct((1, pixels), F32)
    return pl.pallas_call(
        kernel,
        out_shape=(shape, jax.ShapeDtypeStruct((WINDOW, 2, K), F32)) if with_basis else shape,
        in_specs=[SMEM] + [VMEM] * (len(arrays) - 1),
        out_specs=(VMEM, VMEM) if with_basis else VMEM,
        scratch_shapes=[pltpu.VMEM((USED, USED), BF16), pltpu.VMEM((2, USED, CHUNK), BF16)],
        cost_estimate=pl.CostEstimate(flops=flops, bytes_accessed=10**7, transcendentals=0),
        compiler_params=parameters(),
        name=name,
    )(*arrays)


def in_lanes(start):
    rows = start.T
    gap = jnp.zeros((K, 32 - REM), F32)
    rest = jnp.zeros((K, 64), F32)
    return jnp.concatenate(
        [
            rows[:, 0:MAIN],
            rows[:, HALF : HALF + MAIN],
            rows[:, MAIN:HALF],
            gap,
            rows[:, HALF + MAIN :],
            gap,
            rest,
        ],
        axis=1,
    )


def body(iq, tail_frames, start_basis, low_rank, high_rank):
    pixels = iq.shape[-1]
    half = pixels // 2
    core = lax.axis_index("pix_3")
    block = lax.axis_index("tm")
    place = jnp.stack([core, block]).astype(jnp.int32)
    chips = lax.axis_size(PLANE)
    pair = ("pix_3", "tm")

    near = lax.ppermute(picked(place, iq), "tm", [(0, 1), (1, 0)])
    frames = jnp.transpose(iq.reshape(2, HALF, 2, pixels), (2, 0, 1, 3))
    tail = jnp.swapaxes(tail_frames, 0, 1)
    keep, swap, extra, own_half = local_products(place, frames, tail)
    swapped = lax.ppermute(swap, "pix_3", [(0, 1), (1, 0)])
    extra_one = lax.ppermute(extra, pair, [(3, 2)])
    extra_two = lax.ppermute(extra, pair, [(1, 2)])
    near = jnp.swapaxes(near, 0, 1)
    late = cross_products(place, own_half, near)
    one = lax.ppermute(late, pair, [(3, 2)])
    two = lax.ppermute(late, pair, [(1, 2)])
    three = lax.ppermute(late, pair, [(0, 2)])
    mine = merged(place, keep, swapped, extra_one, extra_two, late, one, two, three)
    pieces = lax.all_to_all(mine.reshape(chips, PACKED // chips, 128), PLANE, 0, 0, tiled=True)
    piece = pieces.sum(axis=0)
    piece = piece + lax.ppermute(piece, "pix_0", [(0, 1), (1, 0)])
    packed = lax.all_to_all(
        jnp.broadcast_to(piece[None], pieces.shape), PLANE, 0, 0, tiled=True
    ).reshape(PACKED, 128)
    found = iterate(place, low_rank, high_rank, packed, in_lanes(start_basis))
    one = lax.ppermute(found, pair, [(2, 3)])
    two = lax.ppermute(found, pair, [(2, 1)])
    other = lax.ppermute(found, "pix_3", [(0, 1), (1, 0)])
    flops = 3 * 10**9
    own = power_call(
        own_kernel, "own", pixels, flops, False, place, found, frames, tail
    )
    shared = power_call(
        shared_kernel, "shared", half, flops // 2, False,
        place, found, other, one, two, frames, near,
    )
    back = lax.ppermute(shared, "tm", [(1, 0)])
    rest, basis = power_call(
        other_kernel, "other", pixels, flops, True,
        place, found, other, frames, tail,
    )
    even = jnp.where(core == 0, own, rest)
    odd = jnp.where(core == 0, rest, own)
    odd = jnp.where(block == 0, jnp.concatenate([shared, back], axis=1), odd)
    return jnp.concatenate([even, odd], axis=0), jnp.swapaxes(basis, 0, 1)


def solution(mesh):
    torus = Mesh(
        mesh.devices.reshape(2, 8, 4, 2, mesh.shape["tm"]),
        ("pix_0", "pix_1", "pix_2", "pix_3", "tm"),
    )
    return jax.shard_map(
        body,
        mesh=torus,
        in_specs=(P("tm", None, PIX), P(None, None, PIX), P(), P("tm"), P("tm")),
        out_specs=(P("tm", PIX), P("tm", None, None)),
        check_vma=False,
    )
```

```python
import functools

import jax
import jax.numpy as jnp
from jax import lax
from jax.experimental import pallas as pl
from jax.experimental.pallas import tpu as pltpu
from jax.sharding import Mesh
from jax.sharding import PartitionSpec as P

K = 128
ITERS = 3
WINDOW = 300
HALF = 150
MAIN = 128
REM = HALF - MAIN
SPAN = 384
USED = 320
FLAG = 320
TILE = 32
PACKED = 512
EXTRA = 288
LATE = 184
CHUNK = 1024
LIMIT = 20 * 2**20
HI = lax.Precision.HIGHEST
F32 = jnp.float32
BF16 = jnp.bfloat16
PIX = ("pix_0", "pix_1", "pix_2", "pix_3")
PLANE = ("pix_1", "pix_2")
SMEM = pl.BlockSpec(memory_space=pltpu.SMEM)
VMEM = pl.BlockSpec(memory_space=pltpu.VMEM)


def grid_of(shape, axis):
    return lax.broadcasted_iota(jnp.int32, shape, axis)


def across(a, b):
    return lax.dot_general(a, b, (((1,), (1,)), ((), ())), preferred_element_type=F32)


def parameters():
    return pltpu.CompilerParams(vmem_limit_bytes=LIMIT)


def pick_kernel(source, out, done):
    first = 1 - lax.axis_index("tm")
    width = out.shape[-1]
    copy = pltpu.make_async_copy(
        source.at[
            pl.ds(first * HALF, HALF), :, pl.ds(pl.multiple_of(first * width, 128), width)
        ],
        out,
        done,
    )
    copy.start()
    copy.wait()


def picked(iq):
    half = iq.shape[-1] // 2
    return pl.pallas_call(
        pick_kernel,
        out_shape=jax.ShapeDtypeStruct((HALF, 2, half), iq.dtype),
        in_specs=[pl.BlockSpec(memory_space=pltpu.HBM)],
        out_specs=VMEM,
        scratch_shapes=[pltpu.SemaphoreType.DMA],
        compiler_params=parameters(),
        name="picked",
    )(pltpu.with_memory_space_constraint(iq, pltpu.HBM))


def lower_and_diagonal(block):
    row = grid_of((MAIN, 128), 0)
    lane = grid_of((MAIN, 128), 1)
    diagonal = jnp.where(
        grid_of((8, 128), 0) == 0,
        jnp.sum(jnp.where(lane == row, block, 0.0), axis=0, keepdims=True),
        0.0,
    )
    return jnp.where(lane < row, block, 0.0), diagonal


def packed_rows(first, cross, second):
    row = grid_of((MAIN, 128), 0)
    lane = grid_of((MAIN, 128), 1)
    lower, diagonal = lower_and_diagonal(second[0:MAIN, 0:128])
    corner = jnp.where(lane >= row, first[0:MAIN, 0:128], lower)
    side = (
        first[0:152, 128:256]
        + pltpu.roll(cross[0:152, 128:256], 32, 1)
        + pltpu.roll(second[0:152, 128:256], 64, 1)
    )
    return corner, cross[0:152, 0:128], side, diagonal


def local_kernel(place, frames, tail, keep, swap, extra, mine, sums):
    sums[...] = jnp.zeros_like(sums)
    width = 1024
    half = mine.shape[-1]
    part_of = pl.ds(pl.multiple_of(place[1] * half, 128), half)
    for part in range(2):
        mine[part] = frames[part, 1 - place[1], :, part_of]

    def step(i, carry):
        at = pl.ds(pl.multiple_of(i * width, 128), width)
        for part in range(2):
            a = frames[part, 0, :, at]
            b = frames[part, 1, :, at]
            c = tail[part, :, at]
            for index, (left, right) in enumerate(((a, a), (a, b), (b, b), (b, c), (c, c))):
                sums[index, 0:HALF, 0:HALF] += across(left, right)
        return carry

    lax.fori_loop(0, frames.shape[-1] // width, step, 0)
    core = place[0] == 1
    scale = place[1].astype(F32)
    even = packed_rows(sums[0], sums[1], sums[2])
    odd = packed_rows(sums[2], sums[3] * scale, sums[4] * scale)
    at = 0
    for one, two in zip(even, odd):
        rows = one.shape[0]
        keep[at : at + rows] = jnp.where(core, two, one)
        swap[at : at + rows] = jnp.where(core, one, two)
        at += rows
    keep[440:] = jnp.zeros((PACKED - 440, 128), F32)
    swap[440:] = jnp.zeros((PACKED - 440, 128), F32)
    lower, diagonal = lower_and_diagonal(sums[0, 0:MAIN, 0:128])
    extra[0:MAIN] = lower
    extra[MAIN : MAIN + 152] = pltpu.roll(sums[0, 0:152, 128:256], 64, 1)
    extra[MAIN + 152 : EXTRA] = diagonal


def local_products(place, frames, tail):
    shape = jax.ShapeDtypeStruct((PACKED, 128), F32)
    return pl.pallas_call(
        local_kernel,
        out_shape=(
            shape,
            shape,
            jax.ShapeDtypeStruct((EXTRA, 128), F32),
            jax.ShapeDtypeStruct((2, HALF, frames.shape[-1] // 2), BF16),
        ),
        in_specs=[SMEM, VMEM, VMEM],
        out_specs=(VMEM, VMEM, VMEM, VMEM),
        scratch_shapes=[pltpu.VMEM((5, 152, 256), F32)],
        cost_estimate=pl.CostEstimate(flops=4 * 10**9, bytes_accessed=8 * 10**6, transcendentals=0),
        compiler_params=parameters(),
        name="local_products",
    )(place, frames, tail)


def cross_kernel(place, own, arrived, late, sums):
    total = jnp.zeros((HALF, HALF), F32)
    for part in range(2):
        total += across(own[part], arrived[part])
    sums[...] = jnp.zeros_like(sums)
    sums[0:HALF, 0:HALF] = total

    @pl.when(place[1] == 1)
    def _():
        sums[0:256] = sums[...].T

    late[0:152] = sums[0:152, 0:128]
    side = jnp.zeros((32, 128), F32)
    for g in range(5):
        rows = sums[32 * g : 32 * g + 32, 128:256]
        side += pltpu.roll(rows, 24 * g, 1) if g else rows
    late[152:LATE] = side


def cross_products(place, own, arrived):
    return pl.pallas_call(
        cross_kernel,
        out_shape=jax.ShapeDtypeStruct((LATE, 128), F32),
        in_specs=[SMEM, VMEM, VMEM],
        out_specs=VMEM,
        scratch_shapes=[pltpu.VMEM((256, 256), F32)],
        cost_estimate=pl.CostEstimate(flops=4 * 10**8, bytes_accessed=3 * 10**6, transcendentals=0),
        compiler_params=parameters(),
        name="cross_products",
    )(place, own, arrived)


def merge_kernel(place, keep, swapped, extra_one, extra_two, own, one, two, three, out):
    out[...] = keep[...] + swapped[...]
    extra = extra_one[...] + extra_two[...]
    out[0:MAIN] += extra[0:MAIN]
    out[280:440] += extra[MAIN:EXTRA]

    @pl.when((place[0] == 1) & (place[1] == 0))
    def _():
        late = own[...] + one[...] + two[...] + three[...]
        out[128:280] += late[0:152]
        lane = grid_of((32, 128), 1)
        valid = (lane >= 32) & (lane < 56)
        for g in range(5):
            rows = 24 if g == 4 else 32
            moved = jnp.where(valid, pltpu.roll(late[152:LATE], (32 - 24 * g) % 128, 1), 0.0)
            out[280 + 32 * g : 280 + 32 * g + rows] += moved[0:rows]


def merged(place, *parts):
    return pl.pallas_call(
        merge_kernel,
        out_shape=jax.ShapeDtypeStruct((PACKED, 128), F32),
        in_specs=[SMEM] + [VMEM] * len(parts),
        out_specs=VMEM,
        compiler_params=parameters(),
        name="merged",
    )(place, *parts)


def unpack(rows, gram):
    row = grid_of((128, 128), 0)
    lane = grid_of((128, 128), 1)
    both = rows[0:128]
    turned = both.T
    gram[0:128, 0:128] = jnp.where(lane >= row, both, turned)
    gram[128:256, 128:256] = jnp.where(
        lane < row, both, jnp.where(lane == row, rows[432:433], turned)
    )
    cross = rows[128:256]
    gram[0:128, 128:256] = cross
    gram[128:256, 0:128] = cross.T
    side = rows[280:408]
    turn = jnp.concatenate([rows[256:280], jnp.zeros((104, 128), F32)], axis=0).T
    first = jnp.where(lane < 64, side, 0.0)
    second = jnp.where(lane < 32, turn, jnp.where(lane < 64, pltpu.roll(side, 96, 1), 0.0))
    gram[0:128, 256:384] = first
    gram[128:256, 256:384] = second
    gram[256:384, 0:128] = first.T
    gram[256:384, 128:256] = second.T
    corner = rows[408:432]
    gram[256:384, 256:384] = jnp.zeros((128, 128), F32)
    short = grid_of((24, 128), 1)
    gram[256:280, 256:384] = jnp.where(short < 64, corner, 0.0)
    moved = pltpu.roll(corner, 96, 1)
    square = jnp.concatenate(
        [jnp.where(short < 32, moved, 0.0), jnp.zeros((104, 128), F32)], axis=0
    ).T[0:24]
    gram[288:312, 256:384] = jnp.where(
        short < 32, square, jnp.where(short < 64, moved, 0.0)
    )


def row_of(vector, index):
    return jnp.broadcast_to(vector[index : index + 1, :], vector.shape)


def thirds(x):
    one = x.astype(BF16)
    rest = x - one.astype(F32)
    two = rest.astype(BF16)
    return one, two, (rest - two.astype(F32)).astype(BF16)


def wide_first(x):
    one, two, three = thirds(x)
    group = grid_of(x.shape, 1) // TILE
    head = jnp.where(group == 2, two.astype(F32), one.astype(F32)).astype(BF16)
    tail = jnp.where(
        group == 0, two.astype(F32), jnp.where(group == 1, three.astype(F32), 0.0)
    ).astype(BF16)
    return jnp.concatenate([head, tail], axis=1)


def wide_second(x):
    one, two, three = thirds(x)
    group = grid_of(x.shape, 1) // TILE
    head = jnp.where(
        group == 1, two.astype(F32), jnp.where(group == 3, three.astype(F32), one.astype(F32))
    ).astype(BF16)
    tail = jnp.where(
        group == 0, two.astype(F32), jnp.where(group == 1, one.astype(F32), 0.0)
    ).astype(BF16)
    return jnp.concatenate([head, tail], axis=1)


def tall_second(x):
    one, two, three = thirds(x)
    zero = jnp.zeros((2 * TILE, x.shape[1]), BF16)
    return jnp.concatenate([one, two, one, three, two, one, zero], axis=0)


def eliminate(work, step):
    first = TILE * step
    left = first + TILE
    sub = grid_of((8, 128), 0)
    lane = grid_of((8, 128), 1)
    groups = TILE // 8
    cols = {}
    for g in range(groups):
        top = first + 8 * g
        block = work[top : top + 8, 0:128]
        for k in range(8 * (g + 1)):
            at = first + k
            cols[g, k] = jnp.broadcast_to(block[:, at : at + 1], (8, 128))
    if left < K:
        below = work[left:, 0:128]
        group = grid_of(below.shape, 1) // TILE
        repeated = jnp.zeros_like(below)
        for c in range(4):
            shift = (TILE * (c - step)) % 128
            moved = pltpu.roll(below, shift, 1) if shift else below
            repeated = jnp.where(group == c, moved, repeated)
        under = wide_first(repeated)
    inverse = [
        jnp.where(lane % TILE == sub + 8 * g, 1.0, 0.0).astype(F32) for g in range(groups)
    ]
    for j in range(TILE):
        gj, rj = divmod(j, 8)
        scale = lax.rsqrt(row_of(cols[gj, j], rj))
        for g in range(gj, groups):
            cols[g, j] = cols[g, j] * scale
        for k in range(j + 1, TILE):
            gk, rk = divmod(k, 8)
            factor = row_of(cols[gk, j], rk)
            for g in range(gk, groups):
                cols[g, k] = cols[g, k] - cols[g, j] * factor
        pivot = row_of(inverse[gj], rj) * scale
        for g in range(gj, groups):
            if g == gj:
                below_pivot = jnp.where(sub > rj, cols[g, j], 0.0)
                inverse[g] = jnp.where(sub == rj, pivot, inverse[g] - below_pivot * pivot)
            else:
                inverse[g] = inverse[g] - cols[g, j] * pivot
    turn = jnp.concatenate(inverse, axis=0)
    rows = jnp.dot(
        wide_first(turn), tall_second(work[first:left, :]), preferred_element_type=F32
    )
    work[first:left, :] = rows
    if left < K:
        tall = wide_second(turn)
        factors = across(under, jnp.concatenate([tall] * 4, axis=0))
        work[left:, :] = work[left:, :] - jnp.dot(
            wide_first(factors), tall_second(rows), preferred_element_type=F32
        )


def iterate_kernel(place, low, high, packed, start, basis, gram, work):
    unpack(packed[...], gram)
    work[:, K:] = start[...]

    def step(_, carry):
        image = jnp.dot(work[:, K:], gram[...], precision=HI, preferred_element_type=F32)
        work[:, 0:K] = lax.dot_general(
            image, image, (((1,), (1,)), ((), ())), precision=HI, preferred_element_type=F32
        )
        work[:, K:] = image
        for index in range(K // TILE):
            eliminate(work, index)
        return carry

    lax.fori_loop(0, ITERS, step, 0)
    which = place[0]
    index = grid_of((K, 128), 0)
    kept = (index >= low[which]) & (index < high[which])
    basis[:, 0:256] = work[:, K : K + 256]
    basis[:, 256:384] = jnp.where(
        grid_of((K, 128), 1) == FLAG - 256, jnp.where(kept, 1.0, 0.0), work[:, K + 256 :]
    )


def iterate(place, low, high, packed, start):
    return pl.pallas_call(
        iterate_kernel,
        out_shape=jax.ShapeDtypeStruct((K, SPAN), F32),
        in_specs=[SMEM, SMEM, SMEM, VMEM, VMEM],
        out_specs=VMEM,
        scratch_shapes=[pltpu.VMEM((SPAN, SPAN), F32), pltpu.VMEM((K, K + SPAN), F32)],
        cost_estimate=pl.CostEstimate(flops=14 * 10**9, bytes_accessed=10**6, transcendentals=0),
        compiler_params=pltpu.CompilerParams(vmem_limit_bytes=LIMIT),
        name="iterate",
    )(place, low, high, packed, start)


def projection(rows):
    used = rows[:, 0:USED]
    kept = used * rows[:, FLAG : FLAG + 1]
    return lax.dot_general(
        kept, used, (((0,), (0,)), ((), ())), precision=HI, preferred_element_type=F32
    ).astype(BF16)


def powers(proj, chunk, power, first, second, begin, pixels):
    def step(i, carry):
        at = i * CHUNK
        total = jnp.zeros((1, CHUNK), F32)
        for part in range(2):
            for side, (ref, index, offset) in enumerate((first, second)):
                where = pl.ds(pl.multiple_of(offset + at, 128), CHUNK)
                block = ref[part, :, where] if index is None else ref[part, index, :, where]
                chunk[part, 128 * side : 128 * side + MAIN, :] = block[0:MAIN]
                chunk[part, 256 + 32 * side : 256 + 32 * side + REM, :] = block[MAIN:HALF]
            out = jnp.dot(proj[...], chunk[part], preferred_element_type=F32)
            total += jnp.sum(out * out, axis=0, keepdims=True)
        power[:, pl.ds(pl.multiple_of(begin + at, 128), CHUNK)] = total / WINDOW
        return carry

    lax.fori_loop(0, pixels // CHUNK, step, 0, unroll=2)


def whole_window(place, proj, chunk, power, frames, tail, odd):
    pixels = frames.shape[-1]

    @pl.when(jnp.logical_not(odd))
    def _():
        powers(proj, chunk, power, (frames, 0, 0), (frames, 1, 0), 0, pixels)

    @pl.when(odd & (place[1] == 1))
    def _():
        powers(proj, chunk, power, (frames, 1, 0), (tail, None, 0), 0, pixels)


def own_kernel(place, mine, frames, tail, power, proj, chunk):
    chunk[...] = jnp.zeros_like(chunk)
    proj[...] = projection(mine[...])
    whole_window(place, proj, chunk, power, frames, tail, place[0] == 1)


def shared_kernel(place, mine, other, one, two, frames, near, power, proj, chunk):
    chunk[...] = jnp.zeros_like(chunk)
    pixels = near.shape[-1]
    last = place[1] == 1
    found = jnp.where(
        last, one[...] + two[...], jnp.where(place[0] == 1, mine[...], other[...])
    )
    proj[...] = projection(found)

    @pl.when(last)
    def _():
        powers(proj, chunk, power, (near, None, 0), (frames, 0, pixels), 0, pixels)

    @pl.when(jnp.logical_not(last))
    def _():
        powers(proj, chunk, power, (frames, 1, 0), (near, None, 0), 0, pixels)


def other_kernel(place, mine, other, frames, tail, power, basis, proj, chunk, held, done):
    core = place[0] == 1
    for window in range(2):
        own = core if window else jnp.logical_not(core)
        rows = jnp.where(own, mine[...], other[...])
        ends = rows[:, 256:384].T
        held[0:MAIN, window, :] = rows[:, 0:128].T
        held[MAIN:HALF, window, :] = ends[0:REM]
        held[HALF : HALF + MAIN, window, :] = rows[:, 128:256].T
        held[HALF + MAIN : WINDOW, window, :] = ends[32 : 32 + REM]
    copy = pltpu.make_async_copy(held, basis, done)
    copy.start()
    chunk[...] = jnp.zeros_like(chunk)
    proj[...] = projection(other[...])
    whole_window(place, proj, chunk, power, frames, tail, place[0] == 0)
    copy.wait()


def power_call(kernel, name, pixels, flops, with_basis, *arrays):
    shape = jax.ShapeDtypeStruct((1, pixels), F32)
    scratch = [pltpu.VMEM((USED, USED), BF16), pltpu.VMEM((2, USED, CHUNK), BF16)]
    outs, specs = shape, VMEM
    if with_basis:
        outs = (shape, jax.ShapeDtypeStruct((WINDOW, 2, K), F32))
        specs = (VMEM, pl.BlockSpec(memory_space=pl.ANY))
        scratch += [pltpu.VMEM((WINDOW, 2, K), F32), pltpu.SemaphoreType.DMA]
    return pl.pallas_call(
        kernel,
        out_shape=outs,
        in_specs=[SMEM] + [VMEM] * (len(arrays) - 1),
        out_specs=specs,
        scratch_shapes=scratch,
        cost_estimate=pl.CostEstimate(flops=flops, bytes_accessed=10**7, transcendentals=0),
        compiler_params=parameters(),
        name=name,
    )(*arrays)


def in_lanes(start):
    rows = start.T
    gap = jnp.zeros((K, 32 - REM), F32)
    rest = jnp.zeros((K, 64), F32)
    return jnp.concatenate(
        [
            rows[:, 0:MAIN],
            rows[:, HALF : HALF + MAIN],
            rows[:, MAIN:HALF],
            gap,
            rows[:, HALF + MAIN :],
            gap,
            rest,
        ],
        axis=1,
    )


def body(iq, tail_frames, start_basis, low_rank, high_rank):
    pixels = iq.shape[-1]
    half = pixels // 2
    core = lax.axis_index("pix_3")
    block = lax.axis_index("tm")
    place = jnp.stack([core, block]).astype(jnp.int32)
    chips = lax.axis_size(PLANE)
    pair = ("pix_3", "tm")

    near = lax.ppermute(picked(iq), "tm", [(0, 1), (1, 0)])
    frames = jnp.transpose(iq.reshape(2, HALF, 2, pixels), (2, 0, 1, 3))
    tail = jnp.swapaxes(tail_frames, 0, 1)
    keep, swap, extra, own_half = local_products(place, frames, tail)
    swapped = lax.ppermute(swap, "pix_3", [(0, 1), (1, 0)])
    extra_one = lax.ppermute(extra, pair, [(3, 2)])
    extra_two = lax.ppermute(extra, pair, [(1, 2)])
    near = jnp.swapaxes(near, 0, 1)
    late = cross_products(place, own_half, near)
    one = lax.ppermute(late, pair, [(3, 2)])
    two = lax.ppermute(late, pair, [(1, 2)])
    three = lax.ppermute(late, pair, [(0, 2)])
    mine = merged(place, keep, swapped, extra_one, extra_two, late, one, two, three)
    pieces = lax.all_to_all(mine.reshape(chips, PACKED // chips, 128), PLANE, 0, 0, tiled=True)
    piece = pieces.sum(axis=0)
    piece = piece + lax.ppermute(piece, "pix_0", [(0, 1), (1, 0)])
    packed = lax.all_to_all(
        jnp.broadcast_to(piece[None], pieces.shape), PLANE, 0, 0, tiled=True
    ).reshape(PACKED, 128)
    found = iterate(place, low_rank, high_rank, packed, in_lanes(start_basis))
    one = lax.ppermute(found, pair, [(2, 3)])
    two = lax.ppermute(found, pair, [(2, 1)])
    other = lax.ppermute(found, "pix_3", [(0, 1), (1, 0)])
    flops = 3 * 10**9
    own = power_call(
        own_kernel, "own", pixels, flops, False, place, found, frames, tail
    )
    shared = power_call(
        shared_kernel, "shared", half, flops // 2, False,
        place, found, other, one, two, frames, near,
    )
    back = lax.ppermute(shared, "tm", [(1, 0)])
    rest, basis = power_call(
        other_kernel, "other", pixels, flops, True,
        place, found, other, frames, tail,
    )
    even = jnp.where(core == 0, own, rest)
    odd = jnp.where(core == 0, rest, own)
    odd = jnp.where(block == 0, jnp.concatenate([shared, back], axis=1), odd)
    return jnp.concatenate([even, odd], axis=0), jnp.swapaxes(basis, 0, 1)


def solution(mesh):
    torus = Mesh(
        mesh.devices.reshape(2, 8, 4, 2, mesh.shape["tm"]),
        ("pix_0", "pix_1", "pix_2", "pix_3", "tm"),
    )
    return jax.shard_map(
        body,
        mesh=torus,
        in_specs=(P("tm", None, PIX), P(None, None, PIX), P(), P("tm"), P("tm")),
        out_specs=(P("tm", PIX), P("tm", None, None)),
        check_vma=False,
    )
```

```python
import functools

import jax
import jax.numpy as jnp
from jax import lax
from jax.experimental import pallas as pl
from jax.experimental.pallas import tpu as pltpu
from jax.sharding import Mesh
from jax.sharding import PartitionSpec as P

K = 128
ITERS = 3
WINDOW = 300
HALF = 150
MAIN = 128
REM = HALF - MAIN
SPAN = 384
USED = 320
FLAG = 320
TILE = 32
PACKED = 512
EXTRA = 288
LATE = 184
CHUNK = 1024
LIMIT = 20 * 2**20
HI = lax.Precision.HIGHEST
F32 = jnp.float32
BF16 = jnp.bfloat16
PIX = ("pix_0", "pix_1", "pix_2", "pix_3")
PLANE = ("pix_1", "pix_2")
SMEM = pl.BlockSpec(memory_space=pltpu.SMEM)
VMEM = pl.BlockSpec(memory_space=pltpu.VMEM)


def grid_of(shape, axis):
    return lax.broadcasted_iota(jnp.int32, shape, axis)


def across(a, b):
    return lax.dot_general(a, b, (((1,), (1,)), ((), ())), preferred_element_type=F32)


def parameters():
    return pltpu.CompilerParams(vmem_limit_bytes=LIMIT)


def pick_kernel(source, out, done):
    first = 1 - lax.axis_index("tm")
    width = out.shape[-1]
    copy = pltpu.make_async_copy(
        source.at[
            pl.ds(first * HALF, HALF), :, pl.ds(pl.multiple_of(first * width, 128), width)
        ],
        out,
        done,
    )
    copy.start()
    copy.wait()


def picked(iq):
    half = iq.shape[-1] // 2
    return pl.pallas_call(
        pick_kernel,
        out_shape=jax.ShapeDtypeStruct((HALF, 2, half), iq.dtype),
        in_specs=[pl.BlockSpec(memory_space=pltpu.HBM)],
        out_specs=VMEM,
        scratch_shapes=[pltpu.SemaphoreType.DMA],
        compiler_params=parameters(),
        name="picked",
    )(pltpu.with_memory_space_constraint(iq, pltpu.HBM))


def lower_and_diagonal(block):
    row = grid_of((MAIN, 128), 0)
    lane = grid_of((MAIN, 128), 1)
    diagonal = jnp.where(
        grid_of((8, 128), 0) == 0,
        jnp.sum(jnp.where(lane == row, block, 0.0), axis=0, keepdims=True),
        0.0,
    )
    return jnp.where(lane < row, block, 0.0), diagonal


def packed_rows(first, cross, second):
    row = grid_of((MAIN, 128), 0)
    lane = grid_of((MAIN, 128), 1)
    lower, diagonal = lower_and_diagonal(second[0:MAIN, 0:128])
    corner = jnp.where(lane >= row, first[0:MAIN, 0:128], lower)
    side = (
        first[0:152, 128:256]
        + pltpu.roll(cross[0:152, 128:256], 32, 1)
        + pltpu.roll(second[0:152, 128:256], 64, 1)
    )
    return corner, cross[0:152, 0:128], side, diagonal


def local_kernel(place, frames, tail, keep, swap, extra, mine, sums):
    sums[...] = jnp.zeros_like(sums)
    width = 1024
    half = mine.shape[-1]
    part_of = pl.ds(pl.multiple_of(place[1] * half, 128), half)
    for part in range(2):
        mine[part] = frames[part, 1 - place[1], :, part_of]

    def step(i, carry):
        at = pl.ds(pl.multiple_of(i * width, 128), width)
        for part in range(2):
            a = frames[part, 0, :, at]
            b = frames[part, 1, :, at]
            c = tail[part, :, at]
            for index, (left, right) in enumerate(((a, a), (a, b), (b, b), (b, c), (c, c))):
                sums[index, 0:HALF, 0:HALF] += across(left, right)
        return carry

    lax.fori_loop(0, frames.shape[-1] // width, step, 0)
    core = place[0] == 1
    scale = place[1].astype(F32)
    even = packed_rows(sums[0], sums[1], sums[2])
    odd = packed_rows(sums[2], sums[3] * scale, sums[4] * scale)
    at = 0
    for one, two in zip(even, odd):
        rows = one.shape[0]
        keep[at : at + rows] = jnp.where(core, two, one)
        swap[at : at + rows] = jnp.where(core, one, two)
        at += rows
    keep[440:] = jnp.zeros((PACKED - 440, 128), F32)
    swap[440:] = jnp.zeros((PACKED - 440, 128), F32)
    lower, diagonal = lower_and_diagonal(sums[0, 0:MAIN, 0:128])
    extra[0:MAIN] = lower
    extra[MAIN : MAIN + 152] = pltpu.roll(sums[0, 0:152, 128:256], 64, 1)
    extra[MAIN + 152 : EXTRA] = diagonal


def local_products(place, frames, tail):
    shape = jax.ShapeDtypeStruct((PACKED, 128), F32)
    return pl.pallas_call(
        local_kernel,
        out_shape=(
            shape,
            shape,
            jax.ShapeDtypeStruct((EXTRA, 128), F32),
            jax.ShapeDtypeStruct((2, HALF, frames.shape[-1] // 2), BF16),
        ),
        in_specs=[SMEM, VMEM, VMEM],
        out_specs=(VMEM, VMEM, VMEM, VMEM),
        scratch_shapes=[pltpu.VMEM((5, 152, 256), F32)],
        cost_estimate=pl.CostEstimate(flops=4 * 10**9, bytes_accessed=8 * 10**6, transcendentals=0),
        compiler_params=parameters(),
        name="local_products",
    )(place, frames, tail)


def cross_kernel(place, own, arrived, late, sums):
    total = jnp.zeros((HALF, HALF), F32)
    for part in range(2):
        total += across(own[part], arrived[part])
    sums[...] = jnp.zeros_like(sums)
    sums[0:HALF, 0:HALF] = total

    @pl.when(place[1] == 1)
    def _():
        sums[0:256] = sums[...].T

    late[0:152] = sums[0:152, 0:128]
    side = jnp.zeros((32, 128), F32)
    for g in range(5):
        rows = sums[32 * g : 32 * g + 32, 128:256]
        side += pltpu.roll(rows, 24 * g, 1) if g else rows
    late[152:LATE] = side


def cross_products(place, own, arrived):
    return pl.pallas_call(
        cross_kernel,
        out_shape=jax.ShapeDtypeStruct((LATE, 128), F32),
        in_specs=[SMEM, VMEM, VMEM],
        out_specs=VMEM,
        scratch_shapes=[pltpu.VMEM((256, 256), F32)],
        cost_estimate=pl.CostEstimate(flops=4 * 10**8, bytes_accessed=3 * 10**6, transcendentals=0),
        compiler_params=parameters(),
        name="cross_products",
    )(place, own, arrived)


def merge_kernel(place, keep, swapped, extra_one, extra_two, own, one, two, three, out):
    out[...] = keep[...] + swapped[...]
    extra = extra_one[...] + extra_two[...]
    out[0:MAIN] += extra[0:MAIN]
    out[280:440] += extra[MAIN:EXTRA]

    @pl.when((place[0] == 1) & (place[1] == 0))
    def _():
        late = own[...] + one[...] + two[...] + three[...]
        out[128:280] += late[0:152]
        lane = grid_of((32, 128), 1)
        valid = (lane >= 32) & (lane < 56)
        for g in range(5):
            rows = 24 if g == 4 else 32
            moved = jnp.where(valid, pltpu.roll(late[152:LATE], (32 - 24 * g) % 128, 1), 0.0)
            out[280 + 32 * g : 280 + 32 * g + rows] += moved[0:rows]


def merged(place, *parts):
    return pl.pallas_call(
        merge_kernel,
        out_shape=jax.ShapeDtypeStruct((PACKED, 128), F32),
        in_specs=[SMEM] + [VMEM] * len(parts),
        out_specs=VMEM,
        compiler_params=parameters(),
        name="merged",
    )(place, *parts)


def spread_kernel(one, two, out):
    out[...] = jnp.broadcast_to((one[...] + two[...])[None], out.shape)


def spread(one, two, copies):
    return pl.pallas_call(
        spread_kernel,
        out_shape=jax.ShapeDtypeStruct((copies, *one.shape), F32),
        in_specs=[VMEM, VMEM],
        out_specs=VMEM,
        compiler_params=parameters(),
        name="spread",
    )(one, two)


def unpack(rows, gram):
    row = grid_of((128, 128), 0)
    lane = grid_of((128, 128), 1)
    both = rows[0:128]
    turned = both.T
    gram[0:128, 0:128] = jnp.where(lane >= row, both, turned)
    gram[128:256, 128:256] = jnp.where(
        lane < row, both, jnp.where(lane == row, rows[432:433], turned)
    )
    cross = rows[128:256]
    gram[0:128, 128:256] = cross
    gram[128:256, 0:128] = cross.T
    side = rows[280:408]
    turn = jnp.concatenate([rows[256:280], jnp.zeros((104, 128), F32)], axis=0).T
    first = jnp.where(lane < 64, side, 0.0)
    second = jnp.where(lane < 32, turn, jnp.where(lane < 64, pltpu.roll(side, 96, 1), 0.0))
    gram[0:128, 256:384] = first
    gram[128:256, 256:384] = second
    gram[256:384, 0:128] = first.T
    gram[256:384, 128:256] = second.T
    corner = rows[408:432]
    gram[256:384, 256:384] = jnp.zeros((128, 128), F32)
    short = grid_of((24, 128), 1)
    gram[256:280, 256:384] = jnp.where(short < 64, corner, 0.0)
    moved = pltpu.roll(corner, 96, 1)
    square = jnp.concatenate(
        [jnp.where(short < 32, moved, 0.0), jnp.zeros((104, 128), F32)], axis=0
    ).T[0:24]
    gram[288:312, 256:384] = jnp.where(
        short < 32, square, jnp.where(short < 64, moved, 0.0)
    )


def row_of(vector, index):
    return jnp.broadcast_to(vector[index : index + 1, :], vector.shape)


def thirds(x):
    one = x.astype(BF16)
    rest = x - one.astype(F32)
    two = rest.astype(BF16)
    return one, two, (rest - two.astype(F32)).astype(BF16)


def wide_first(x):
    one, two, three = thirds(x)
    group = grid_of(x.shape, 1) // TILE
    head = jnp.where(group == 2, two.astype(F32), one.astype(F32)).astype(BF16)
    tail = jnp.where(
        group == 0, two.astype(F32), jnp.where(group == 1, three.astype(F32), 0.0)
    ).astype(BF16)
    return jnp.concatenate([head, tail], axis=1)


def wide_second(x):
    one, two, three = thirds(x)
    group = grid_of(x.shape, 1) // TILE
    head = jnp.where(
        group == 1, two.astype(F32), jnp.where(group == 3, three.astype(F32), one.astype(F32))
    ).astype(BF16)
    tail = jnp.where(
        group == 0, two.astype(F32), jnp.where(group == 1, one.astype(F32), 0.0)
    ).astype(BF16)
    return jnp.concatenate([head, tail], axis=1)


def tall_second(x):
    one, two, three = thirds(x)
    zero = jnp.zeros((2 * TILE, x.shape[1]), BF16)
    return jnp.concatenate([one, two, one, three, two, one, zero], axis=0)


def eliminate(work, step):
    first = TILE * step
    left = first + TILE
    sub = grid_of((8, 128), 0)
    lane = grid_of((8, 128), 1)
    groups = TILE // 8
    cols = {}
    for g in range(groups):
        top = first + 8 * g
        block = work[top : top + 8, 0:128]
        for k in range(8 * (g + 1)):
            at = first + k
            cols[g, k] = jnp.broadcast_to(block[:, at : at + 1], (8, 128))
    if left < K:
        below = work[left:, 0:128]
        group = grid_of(below.shape, 1) // TILE
        repeated = jnp.zeros_like(below)
        for c in range(4):
            shift = (TILE * (c - step)) % 128
            moved = pltpu.roll(below, shift, 1) if shift else below
            repeated = jnp.where(group == c, moved, repeated)
        under = wide_first(repeated)
    inverse = [
        jnp.where(lane % TILE == sub + 8 * g, 1.0, 0.0).astype(F32) for g in range(groups)
    ]
    for j in range(TILE):
        gj, rj = divmod(j, 8)
        scale = lax.rsqrt(row_of(cols[gj, j], rj))
        for g in range(gj, groups):
            cols[g, j] = cols[g, j] * scale
        for k in range(j + 1, TILE):
            gk, rk = divmod(k, 8)
            factor = row_of(cols[gk, j], rk)
            for g in range(gk, groups):
                cols[g, k] = cols[g, k] - cols[g, j] * factor
        pivot = row_of(inverse[gj], rj) * scale
        for g in range(gj, groups):
            if g == gj:
                below_pivot = jnp.where(sub > rj, cols[g, j], 0.0)
                inverse[g] = jnp.where(sub == rj, pivot, inverse[g] - below_pivot * pivot)
            else:
                inverse[g] = inverse[g] - cols[g, j] * pivot
    turn = jnp.concatenate(inverse, axis=0)
    rows = jnp.dot(
        wide_first(turn), tall_second(work[first:left, :]), preferred_element_type=F32
    )
    work[first:left, :] = rows
    if left < K:
        tall = wide_second(turn)
        factors = across(under, jnp.concatenate([tall] * 4, axis=0))
        work[left:, :] = work[left:, :] - jnp.dot(
            wide_first(factors), tall_second(rows), preferred_element_type=F32
        )


FIRST = (0, 0, 1, 0, 1, 2)
SECOND = (0, 1, 0, 2, 1, 0)


def iterate_kernel(place, low, high, packed, start, basis, gram, work, deep):
    unpack(packed[...], gram)
    split = thirds(gram[...])
    for block, index in enumerate(SECOND):
        deep[SPAN * block : SPAN * (block + 1), :] = split[index]
    work[:, K:] = start[...]

    def step(_, carry):
        split = thirds(work[:, K:])
        image = jnp.dot(
            jnp.concatenate([split[index] for index in FIRST], axis=1),
            deep[...],
            preferred_element_type=F32,
        )
        split = thirds(image)
        work[:, 0:K] = across(
            jnp.concatenate([split[index] for index in FIRST], axis=1),
            jnp.concatenate([split[index] for index in SECOND], axis=1),
        )
        work[:, K:] = image
        for index in range(K // TILE):
            eliminate(work, index)
        return carry

    lax.fori_loop(0, ITERS, step, 0)
    which = place[0]
    index = grid_of((K, 128), 0)
    kept = (index >= low[which]) & (index < high[which])
    basis[:, 0:256] = work[:, K : K + 256]
    basis[:, 256:384] = jnp.where(
        grid_of((K, 128), 1) == FLAG - 256, jnp.where(kept, 1.0, 0.0), work[:, K + 256 :]
    )


def iterate(place, low, high, packed, start):
    return pl.pallas_call(
        iterate_kernel,
        out_shape=jax.ShapeDtypeStruct((K, SPAN), F32),
        in_specs=[SMEM, SMEM, SMEM, VMEM, VMEM],
        out_specs=VMEM,
        scratch_shapes=[
            pltpu.VMEM((SPAN, SPAN), F32),
            pltpu.VMEM((K, K + SPAN), F32),
            pltpu.VMEM((len(SECOND) * SPAN, SPAN), BF16),
        ],
        cost_estimate=pl.CostEstimate(flops=14 * 10**9, bytes_accessed=10**6, transcendentals=0),
        compiler_params=pltpu.CompilerParams(vmem_limit_bytes=LIMIT),
        name="iterate",
    )(place, low, high, packed, start)


def projection(rows):
    used = rows[:, 0:USED]
    kept = used * rows[:, FLAG : FLAG + 1]
    return lax.dot_general(
        kept, used, (((0,), (0,)), ((), ())), precision=HI, preferred_element_type=F32
    ).astype(BF16)


def powers(proj, chunk, power, first, second, begin, pixels):
    def step(i, carry):
        at = i * CHUNK
        total = jnp.zeros((1, CHUNK), F32)
        for part in range(2):
            for side, (ref, index, offset) in enumerate((first, second)):
                where = pl.ds(pl.multiple_of(offset + at, 128), CHUNK)
                block = ref[part, :, where] if index is None else ref[part, index, :, where]
                chunk[part, 128 * side : 128 * side + MAIN, :] = block[0:MAIN]
                chunk[part, 256 + 32 * side : 256 + 32 * side + REM, :] = block[MAIN:HALF]
            out = jnp.dot(proj[0:312], chunk[part], preferred_element_type=F32)
            total += jnp.sum(out * out, axis=0, keepdims=True)
        power[:, pl.ds(pl.multiple_of(begin + at, 128), CHUNK)] = total / WINDOW
        return carry

    lax.fori_loop(0, pixels // CHUNK, step, 0, unroll=2)


def whole_window(place, proj, chunk, power, frames, tail, odd):
    pixels = frames.shape[-1]

    @pl.when(jnp.logical_not(odd))
    def _():
        powers(proj, chunk, power, (frames, 0, 0), (frames, 1, 0), 0, pixels)

    @pl.when(odd & (place[1] == 1))
    def _():
        powers(proj, chunk, power, (frames, 1, 0), (tail, None, 0), 0, pixels)


def own_kernel(place, mine, frames, tail, power, proj, chunk):
    chunk[...] = jnp.zeros_like(chunk)
    proj[...] = projection(mine[...])
    whole_window(place, proj, chunk, power, frames, tail, place[0] == 1)


def shared_kernel(place, mine, other, one, two, frames, near, power, proj, chunk):
    chunk[...] = jnp.zeros_like(chunk)
    pixels = near.shape[-1]
    last = place[1] == 1
    found = jnp.where(
        last, one[...] + two[...], jnp.where(place[0] == 1, mine[...], other[...])
    )
    proj[...] = projection(found)

    @pl.when(last)
    def _():
        powers(proj, chunk, power, (near, None, 0), (frames, 0, pixels), 0, pixels)

    @pl.when(jnp.logical_not(last))
    def _():
        powers(proj, chunk, power, (frames, 1, 0), (near, None, 0), 0, pixels)


def other_kernel(place, mine, other, frames, tail, power, basis, proj, chunk, held, done):
    core = place[0] == 1
    for window in range(2):
        own = core if window else jnp.logical_not(core)
        rows = jnp.where(own, mine[...], other[...])
        ends = rows[:, 256:384].T
        held[0:MAIN, window, :] = rows[:, 0:128].T
        held[MAIN:HALF, window, :] = ends[0:REM]
        held[HALF : HALF + MAIN, window, :] = rows[:, 128:256].T
        held[HALF + MAIN : WINDOW, window, :] = ends[32 : 32 + REM]
    copy = pltpu.make_async_copy(held, basis, done)
    copy.start()
    chunk[...] = jnp.zeros_like(chunk)
    proj[...] = projection(other[...])
    whole_window(place, proj, chunk, power, frames, tail, place[0] == 0)
    copy.wait()


def power_call(kernel, name, pixels, flops, with_basis, *arrays):
    shape = jax.ShapeDtypeStruct((1, pixels), F32)
    scratch = [pltpu.VMEM((USED, USED), BF16), pltpu.VMEM((2, USED, CHUNK), BF16)]
    outs, specs = shape, VMEM
    if with_basis:
        outs = (shape, jax.ShapeDtypeStruct((WINDOW, 2, K), F32))
        specs = (VMEM, pl.BlockSpec(memory_space=pl.ANY))
        scratch += [pltpu.VMEM((WINDOW, 2, K), F32), pltpu.SemaphoreType.DMA]
    return pl.pallas_call(
        kernel,
        out_shape=outs,
        in_specs=[SMEM] + [VMEM] * (len(arrays) - 1),
        out_specs=specs,
        scratch_shapes=scratch,
        cost_estimate=pl.CostEstimate(flops=flops, bytes_accessed=10**7, transcendentals=0),
        compiler_params=parameters(),
        name=name,
    )(*arrays)


def in_lanes(start):
    rows = start.T
    gap = jnp.zeros((K, 32 - REM), F32)
    rest = jnp.zeros((K, 64), F32)
    return jnp.concatenate(
        [
            rows[:, 0:MAIN],
            rows[:, HALF : HALF + MAIN],
            rows[:, MAIN:HALF],
            gap,
            rows[:, HALF + MAIN :],
            gap,
            rest,
        ],
        axis=1,
    )


def body(iq, tail_frames, start_basis, low_rank, high_rank):
    pixels = iq.shape[-1]
    half = pixels // 2
    core = lax.axis_index("pix_3")
    block = lax.axis_index("tm")
    place = jnp.stack([core, block]).astype(jnp.int32)
    chips = lax.axis_size(PLANE)
    pair = ("pix_3", "tm")

    near = lax.ppermute(picked(iq), "tm", [(0, 1), (1, 0)])
    frames = jnp.transpose(iq.reshape(2, HALF, 2, pixels), (2, 0, 1, 3))
    tail = jnp.swapaxes(tail_frames, 0, 1)
    keep, swap, extra, own_half = local_products(place, frames, tail)
    swapped = lax.ppermute(swap, "pix_3", [(0, 1), (1, 0)])
    extra_one = lax.ppermute(extra, pair, [(3, 2)])
    extra_two = lax.ppermute(extra, pair, [(1, 2)])
    near = jnp.swapaxes(near, 0, 1)
    late = cross_products(place, own_half, near)
    one = lax.ppermute(late, pair, [(3, 2)])
    two = lax.ppermute(late, pair, [(1, 2)])
    three = lax.ppermute(late, pair, [(0, 2)])
    mine = merged(place, keep, swapped, extra_one, extra_two, late, one, two, three)
    pieces = lax.all_to_all(mine.reshape(chips, PACKED // chips, 128), PLANE, 0, 0, tiled=True)
    piece = pieces.sum(axis=0)
    copies = spread(piece, lax.ppermute(piece, "pix_0", [(0, 1), (1, 0)]), chips)
    packed = lax.all_to_all(copies, PLANE, 0, 0, tiled=True).reshape(PACKED, 128)
    found = iterate(place, low_rank, high_rank, packed, in_lanes(start_basis))
    one = lax.ppermute(found, pair, [(2, 3)])
    two = lax.ppermute(found, pair, [(2, 1)])
    other = lax.ppermute(found, "pix_3", [(0, 1), (1, 0)])
    flops = 3 * 10**9
    own = power_call(
        own_kernel, "own", pixels, flops, False, place, found, frames, tail
    )
    shared = power_call(
        shared_kernel, "shared", half, flops // 2, False,
        place, found, other, one, two, frames, near,
    )
    back = lax.ppermute(shared, "tm", [(1, 0)])
    rest, basis = power_call(
        other_kernel, "other", pixels, flops, True,
        place, found, other, frames, tail,
    )
    even = jnp.where(core == 0, own, rest)
    odd = jnp.where(core == 0, rest, own)
    odd = jnp.where(block == 0, jnp.concatenate([shared, back], axis=1), odd)
    return jnp.concatenate([even, odd], axis=0), jnp.swapaxes(basis, 0, 1)


def solution(mesh):
    torus = Mesh(
        mesh.devices.reshape(2, 8, 4, 2, mesh.shape["tm"]),
        ("pix_0", "pix_1", "pix_2", "pix_3", "tm"),
    )
    return jax.shard_map(
        body,
        mesh=torus,
        in_specs=(P("tm", None, PIX), P(None, None, PIX), P(), P("tm"), P("tm")),
        out_specs=(P("tm", PIX), P("tm", None, None)),
        check_vma=False,
    )
```
